128 devices in a mesh: sph: 16 (over x_lo, z, core), rad: 8 (over y, x_hi).
Axes of the slice: x: 4 (x_hi: 2, x_lo: 2; x = x_hi * 2 + x_lo), y: 4, z: 4, core: 2. Of those that a mesh axis runs over, the one named last changes fastest.
Arguments:
- coeffs: bfloat16 [65536, 480], P('sph'), may hold values from -6 to 6
- interp: bfloat16 [65536, 2048], P('sph', 'rad'), may hold values from -0.055664062 to 0.055664062
- phases: float32 [64, 2048], P(None, 'rad'), may hold values from 0.3 to 3
- tables: bfloat16 [16, 480, 480], P('rad'), may hold values from -0.25 to 0.25
- bins: int32 [65536], P('sph'), may hold values from 0 to 63
Outputs:
- fields: bfloat16 [65536, 480], P('sph', 'rad')
The draws below stay inside these ranges and needn't reach their ends.
All inputs are finite; a program needn't handle non-finite values.
Results may differ from the reference program's by a relative error of at most 0.024.
Values may be sent and summed in bfloat16 or wider, within the bound.
A program may use at most 64 MiB of HBM per device.

```python
import math
import jax
import jax.numpy as jnp
from jax import lax

C = 240
C2 = 480
R = 2048
TBL = 128
NB = 16
NH = 64
S_DEV = 4096
S = 65536
N_SPH = 16


def with_ends(drawn, key, low, top_value):
    longest = drawn.shape.index(max(drawn.shape))
    spots = []
    for shift in (0, 1):
        where = [jax.random.randint(jax.random.fold_in(key, axis), (), 0, length) for axis, length in enumerate(drawn.shape)]
        where[longest] = (where[longest] + shift) % drawn.shape[longest]
        spots.append(tuple(where))
    return drawn.at[spots[0]].set(low).at[spots[1]].set(top_value)


def steps_of(own_key, dims, pieces, low, high):
    def one(axis_at, blocks):
        draws = jax.random.uniform(jax.random.fold_in(jax.random.fold_in(own_key, 6), axis_at), (blocks,), jnp.float32, low / len(pieces), high / len(pieces))
        return jnp.repeat(jnp.exp(draws), dims[axis_at] // blocks).reshape((-1,) + (1,) * (len(dims) - axis_at - 1))

    factor_of = one(*pieces[0])
    for cut in pieces[1:]:
        factor_of = factor_of * one(*cut)
    return factor_of


def noise(key, shape, deviation, reach, pieces=(), held_as=jnp.bfloat16):
    entries = deviation * jax.random.normal(key, shape, jnp.float32)
    if pieces:
        entries = entries * steps_of(key, shape, pieces, -0.22, 0.18)
    return jnp.clip(entries, -reach, reach).astype(held_as)


def setup_inputs(seed: int = 0) -> dict:
    arg_keys = jax.random.split(jax.random.key(seed), 6)
    return {
        "coeffs": noise(arg_keys[0], (S, C2), 1.0, 6.0, ((0, 16),)),
        "interp": noise(arg_keys[1], (S, R), ((S_DEV * N_SPH * R) ** -0.25), 0.055664062, ((0, 16), (1, 8))),
        "phases": jnp.clip(jnp.exp(math.log(3.0) - 2.3025851 * jax.random.uniform(arg_keys[2], (NH, R), jnp.float32) ** steps_of(arg_keys[2], (NH, R), ((1, 8),), -0.2, 0.2)), 0.3, 3.0),
        "tables": noise(arg_keys[3], (NB, C2, C2), (2 * C) ** -0.5, 0.25, ((0, 8),)),
        "bins": with_ends(jax.random.randint(arg_keys[4], (S,), 0, NH), jax.random.fold_in(arg_keys[4], 1), 0, NH - 1).astype(jnp.int32),
    }


def reference(coeffs, interp, phases, tables, bins):
    lifted = phases[bins]
    proj = (interp.astype(jnp.float32) * lifted).astype(jnp.bfloat16)
    nodes_sum = jnp.dot(proj.T, coeffs, preferred_element_type=jnp.float32)
    nodes = nodes_sum.astype(jnp.bfloat16)
    blocks = nodes.reshape(tables.shape[0], TBL, tables.shape[1]).astype(jnp.float32)
    angular = jnp.einsum("btc,bcd->btd", blocks, tables.astype(jnp.float32), precision=lax.Precision.HIGHEST)
    angular = angular.reshape(nodes.shape[0], nodes.shape[1]).astype(jnp.bfloat16)
    return jnp.dot(proj, angular, preferred_element_type=jnp.float32).astype(jnp.bfloat16)
```

```python
import functools

import jax
import jax.numpy as jnp
from jax import lax
from jax.experimental import pallas as pl
from jax.experimental.pallas import tpu as pltpu
from jax.sharding import PartitionSpec as P

MESH = pl.DeviceIdType.MESH
BF = jnp.bfloat16
F32 = jnp.float32

OFF = [(2, 1), (2, 0), (1, 1), (1, 0), (3, 1), (3, 0), (0, 1), (0, 0)]
XK = [k for k, (dy, dx) in enumerate(OFF) if dx]
NQ = [4 if dx else 2 for dy, dx in OFF[:7]]
BASE = [sum(NQ[:k]) for k in range(7)]
NPIECE = sum(NQ)
FIRST = {0: 2, 1: 2, 2: 2, 3: 2, 4: 1, 5: 2, 6: 1}
SECOND = [(4, 1), (6, 1)]
THIRD = [(k, q) for q in (2, 3) for k in XK]


def where():
    s, r = lax.axis_index("sph"), lax.axis_index("rad")
    return (r % 2) * 2 + s // 8, r // 2, (s // 2) % 4, s % 2


def device(x, y, z, c):
    x, y, z, c = x % 4, y % 4, z % 4, c % 2
    return (x % 2) * 8 + z * 2 + c, y * 2 + x // 2


def kernel(
    coeffs, interp, phases, tables, bins, out,
    interp_v, coeffs_v, phases_v, bins_v, table_v, phl_v, perm_v, proj_v, recv_v, acc_v, part_v,
    rs_v, xs_v, xr_v, ang_v, fsend_v, frecv_v, out_v,
    in_sem, co_sem, small_sem, ps_sem, pr_sem, rss_sem, rsr_sem, xx_sem, pls_sem, plr_sem,
    zs_sem, zr_sem, cs_sem, cr_sem, fs_sem, fr_sem, out_sem,
):
    x, y, z, c = where()
    xh, xl = x // 2, x % 2
    rad, slot = y * 2 + xh, z * 2 + c
    rows = pl.multiple_of(slot * 32, 32)

    def chunk_of(k):
        dy, dx = OFF[k]
        return ((y + dy) % 4) * 2 + (xh + dx) % 2

    loads = [
        pltpu.make_async_copy(phases, phases_v, small_sem.at[0]),
        pltpu.make_async_copy(bins, bins_v, small_sem.at[1]),
    ]
    inters, coefs = [], []
    for k in range(8):
        at = pl.ds(pl.multiple_of(chunk_of(k) * 512, 512), 512)
        inters.append(pltpu.make_async_copy(interp.at[at, :], interp_v.at[k], in_sem.at[k]))
        coefs.append(pltpu.make_async_copy(coeffs.at[at, :], coeffs_v.at[k], co_sem.at[k]))
    table = pltpu.make_async_copy(tables.at[slot // 4], table_v, small_sem.at[2])
    for load in [*loads, *inters, *coefs, table]:
        load.start()

    partners = [(x + 2 * dx, y + dy, z, c) for dy, dx in OFF[:7]]
    partners += [(x, y, z + dz, c + dc) for dz in range(4) for dc in range(2) if dz or dc]
    partners += [(x + 1 - 2 * xl, y, z, c)]
    partners += [(3 - x, y + dy, z, c) for dy in range(4)]
    barrier = pltpu.get_barrier_semaphore()
    for partner in partners:
        pl.semaphore_signal(barrier, inc=1, device_id=device(*partner), device_id_type=MESH)

    for load in loads:
        load.wait()
    ph = phases_v[...]
    hi = ph.astype(BF)
    phl_v[0:64, :] = hi
    phl_v[64:128, :] = (ph - hi.astype(F32)).astype(BF)

    def send(src, dst, ssem, rsem, to):
        return pltpu.make_async_remote_copy(
            src_ref=src, dst_ref=dst, send_sem=ssem, recv_sem=rsem, device_id=device(*to), device_id_type=MESH
        )

    def piece(k, q):
        dy, dx = OFF[k]
        n = 512 // NQ[k]
        at = pl.ds(q * n, n)
        cols = pl.ds(pl.multiple_of(rad * 256, 256), 256)
        i = BASE[k] + q
        return send(proj_v.at[k, at, :], recv_v.at[at, cols], ps_sem.at[i], pr_sem.at[i], (x + 2 * dx, y + dy, z, c))

    for k in range(8):
        inters[k].wait()
        at = pl.ds(pl.multiple_of(chunk_of(k) * 512, 512), 512)
        which = bins_v[at][None, :]
        hot = ((lax.broadcasted_iota(jnp.int32, (128, 512), 0) & 63) == which).astype(F32).astype(BF)
        lifted = lax.dot_general(hot, phl_v[...], (((0,), (0,)), ((), ())), preferred_element_type=F32)
        proj_v[k] = (interp_v[k].astype(F32) * lifted).astype(BF)
        if k == 0:
            pl.semaphore_wait(barrier, len(partners))
        if k < 7:
            for q in range(FIRST[k]):
                piece(k, q).start()
        else:
            recv_v[:, pl.ds(pl.multiple_of(rad * 256, 256), 256)] = proj_v[k]

    for k in range(8):
        coefs[k].wait()
        got = lax.dot_general(proj_v[k], coeffs_v[k], (((0,), (0,)), ((), ())), preferred_element_type=F32)
        if k == 0:
            acc_v[...] = got
        else:
            acc_v[...] += got
    part_v[...] = acc_v[...].astype(BF)

    zc = [(dz, dc) for dz in (2, 1, 3, 0) for dc in (0, 1) if dz or dc]
    sums = []
    for i, (dz, dc) in enumerate(zc):
        to_slot = ((z + dz) % 4) * 2 + (c + dc) % 2
        src = part_v.at[pl.ds(pl.multiple_of(to_slot * 32, 32), 32), :]
        sums.append(send(src, rs_v.at[i], rss_sem.at[i], rsr_sem.at[i], (x, y, z + dz, c + dc)))
        sums[-1].start()
    a = lax.broadcasted_iota(jnp.int32, (480, 512), 0)
    b = lax.broadcasted_iota(jnp.int32, (480, 512), 1)
    low = b & 63
    perm_v[...] = jnp.where(low < 60, (a == (b >> 6) * 60 + low).astype(F32), 0.0).astype(BF)
    total = part_v[pl.ds(rows, 32), :].astype(F32)
    for i in range(7):
        sums[i].wait_recv()
        total = total + rs_v[i].astype(F32)
    xs_v[...] = total.astype(BF)
    pair = send(xs_v, xr_v, xx_sem.at[0], xx_sem.at[1], (x + 1 - 2 * xl, y, z, c))
    pair.start()
    for k, q in SECOND:
        piece(k, q).start()
    table.wait()
    pair.wait_recv()
    nodes = (xs_v[...].astype(F32) + xr_v[...].astype(F32)).astype(BF)
    turned = jnp.dot(nodes, table_v[...], preferred_element_type=F32).astype(BF)
    ang_v[y, xh, pl.ds(rows, 32), :] = jnp.dot(turned, perm_v[...], preferred_element_type=F32).astype(BF)

    own = ang_v.at[y, xh, pl.ds(rows, 32), :]
    plane = []
    for i, (flip, dy) in enumerate([(0, 2), (0, 1), (0, 3), (1, 2), (1, 1), (1, 3), (1, 0)]):
        to = (3 - x if flip else x, y + dy, z, c)
        plane.append(send(own, own, pls_sem.at[i], plr_sem.at[i], to))
        plane[-1].start()
    for k, q in THIRD:
        piece(k, q).start()

    def group(g, dz):
        at = pl.multiple_of((((z + dz) % 4) * 2 + c) * 32, 32)
        return ang_v.at[:, (xh + g) % 2, pl.ds(at, 32), :]

    def other_core(g, dz):
        i = g * 4 + dz
        return send(group(g, dz), group(g, dz), cs_sem.at[i], cr_sem.at[i], (x, y, z, c + 1))

    def along(g, dz, step):
        i = g * 3 + (0 if step > 0 else 1) if dz == 0 else g * 3 + 2
        return send(group(g, dz), group(g, dz), zs_sem.at[i], zr_sem.at[i], (x, y, z + step, c))

    ups = {}
    for g in range(2):
        for i in ((0, 1, 2) if g == 0 else (3, 4, 5, 6)):
            plane[i].wait_recv()
        for step in (1, -1):
            ups[g, step] = along(g, 0, step)
            ups[g, step].start()
        ups[g, 0] = other_core(g, 0)
        ups[g, 0].start()
    for g in range(2):
        far = -1 if g == 0 else 1
        ups[g, far].wait_recv()
        back = 1 if g == 0 else -1
        relay = along(g, back, far)
        relay.start()
        ups[g, 2] = relay
        ups[g, 3] = other_core(g, back % 4)
        ups[g, 3].start()
    for g in range(2):
        far = 1 if g == 0 else -1
        ups[g, far].wait_recv()
        ups[g, 4] = other_core(g, (-far) % 4)
        ups[g, 4].start()
    for g in range(2):
        ups[g, 2].wait_recv()
        ups[g, 5] = other_core(g, 2)
        ups[g, 5].start()
    for g in range(2):
        for i in (0, 3, 4, 5):
            ups[g, i].wait_recv()

    for k in range(7):
        for q in range(NQ[k]):
            piece(k, q).wait_recv()
    lane = lax.broadcasted_iota(jnp.int32, (256, 128), 1)
    sent = {}
    for half in range(2):
        cols = ang_v[:, :, :, 256 * half : 256 * half + 256].reshape(2048, 256)
        res = jnp.dot(recv_v[...], cols, preferred_element_type=F32)
        for t in range(2):
            top, bottom = res[:256, 128 * t : 128 * t + 128], res[256:, 128 * t : 128 * t + 128]
            d = 4 * half + 2 * t
            fsend_v[d] = jnp.where(lane < 64, top, pltpu.roll(bottom, 64, 1)).astype(BF)
            fsend_v[d + 1] = jnp.where(lane < 64, pltpu.roll(top, 64, 1), bottom).astype(BF)
    for k in range(7):
        dy, dx = OFF[k]
        sent[k] = send(fsend_v.at[chunk_of(k)], frecv_v.at[k], fs_sem.at[k], fr_sem.at[k], (x + 2 * dx, y + dy, z, c))
        sent[k].start()
    outs = []
    for k in (7, 6, 5, 3, 4, 2, 1, 0):
        dy, dx = OFF[k]
        if k < 7:
            sent[k].wait_recv()
            block = frecv_v[k]
        else:
            block = fsend_v[rad]
        source = ((y - dy) % 4) * 2 + (xh + dx) % 2
        at = pl.multiple_of(source * 512, 512)
        wide = block.astype(F32)
        out_v[pl.ds(at, 256), :] = block[:, :60]
        out_v[pl.ds(at + 256, 256), :] = pltpu.roll(wide, 64, 1).astype(BF)[:, :60]
        outs.append(pltpu.make_async_copy(out_v.at[pl.ds(at, 512), :], out.at[pl.ds(at, 512), :], out_sem.at[k]))
        outs[-1].start()

    for k in range(7):
        for q in range(NQ[k]):
            piece(k, q).wait_send()
        sums[k].wait_send()
        plane[k].wait_send()
        sent[k].wait_send()
    pair.wait_send()
    for copy in ups.values():
        copy.wait_send()
    for copy in outs:
        copy.wait()


def body(coeffs, interp, phases, tables, bins):
    dma = pltpu.SemaphoreType.DMA
    return pl.pallas_call(
        kernel,
        name="coupling",
        out_shape=jax.ShapeDtypeStruct((4096, 60), BF),
        in_specs=[pl.BlockSpec(memory_space=pl.ANY)] * 5,
        out_specs=pl.BlockSpec(memory_space=pl.ANY),
        scratch_shapes=[
            pltpu.VMEM((8, 512, 256), BF),
            pltpu.VMEM((8, 512, 480), BF),
            pltpu.VMEM((64, 256), F32),
            pltpu.VMEM((4096,), jnp.int32),
            pltpu.VMEM((480, 480), BF),
            pltpu.VMEM((128, 256), BF),
            pltpu.VMEM((480, 512), BF),
            pltpu.VMEM((8, 512, 256), BF),
            pltpu.VMEM((512, 2048), BF),
            pltpu.VMEM((256, 480), F32),
            pltpu.VMEM((256, 480), BF),
            pltpu.VMEM((7, 32, 480), BF),
            pltpu.VMEM((32, 480), BF),
            pltpu.VMEM((32, 480), BF),
            pltpu.VMEM((4, 2, 256, 512), BF),
            pltpu.VMEM((8, 256, 128), BF),
            pltpu.VMEM((7, 256, 128), BF),
            pltpu.VMEM((4096, 60), BF),
            dma((8,)), dma((8,)), dma((3,)), dma((NPIECE,)), dma((NPIECE,)), dma((7,)), dma((7,)), dma((2,)),
            dma((7,)), dma((7,)), dma((6,)), dma((6,)), dma((8,)), dma((8,)), dma((7,)), dma((7,)), dma((8,)),
        ],
        compiler_params=pltpu.CompilerParams(
            collective_id=0, has_side_effects=True, vmem_limit_bytes=60 * 1024 * 1024
        ),
    )(coeffs, interp, phases, tables, bins)


def solution(mesh):
    return jax.shard_map(
        body,
        mesh=mesh,
        in_specs=(P("sph", None), P("sph", "rad"), P(None, "rad"), P("rad", None, None), P("sph")),
        out_specs=P("sph", "rad"),
        check_vma=False,
    )
```

```python
import functools

import jax
import jax.numpy as jnp
from jax import lax
from jax.experimental import pallas as pl
from jax.experimental.pallas import tpu as pltpu
from jax.sharding import PartitionSpec as P

MESH = pl.DeviceIdType.MESH
BF = jnp.bfloat16
F32 = jnp.float32

OFF = [(2, 1), (2, 0), (1, 1), (1, 0), (3, 1), (3, 0), (0, 1), (0, 0)]
XK = [k for k, (dy, dx) in enumerate(OFF) if dx]
NQ = [4 if dx else 2 for dy, dx in OFF[:7]]
BASE = [sum(NQ[:k]) for k in range(7)]
NPIECE = sum(NQ)
FIRST = {0: 2, 1: 1, 2: 2, 3: 1, 4: 1, 5: 1, 6: 1}
SECOND = [(4, 1), (6, 1)]
REST = [(0, 2), (2, 2), (1, 1), (4, 2), (6, 2), (3, 1), (0, 3), (2, 3), (5, 1), (4, 3), (6, 3)]
THIRD = {3: REST[:3], 7: REST[3:]}
PLANE = [(0, 0), (0, 1), (0, 3), (1, 0), (0, 2), (1, 1), (1, 3), (1, 2)]
LAG = 8


def where():
    s, r = lax.axis_index("sph"), lax.axis_index("rad")
    return (r % 2) * 2 + s // 8, r // 2, (s // 2) % 4, s % 2


def device(x, y, z, c):
    x, y, z, c = x % 4, y % 4, z % 4, c % 2
    return (x % 2) * 8 + z * 2 + c, y * 2 + x // 2


def kernel(
    coeffs, interp, phases, tables, bins, out,
    interp_v, coeffs_v, phases_v, bins_v, table_v, phl_v, perm_v, proj_v, recv_v, acc_v, part_v,
    rs_v, xs_v, xr_v, ang_v, fsend_v, frecv_v, out_v,
    in_sem, co_sem, small_sem, ps_sem, pr_sem, rss_sem, rsr_sem, xx_sem, pls_sem, plr_sem,
    zs_sem, zr_sem, cs_sem, cr_sem, fs_sem, fr_sem, out_sem,
):
    x, y, z, c = where()
    xh, xl = x // 2, x % 2
    rad, slot = y * 2 + xh, z * 2 + c
    rows = pl.multiple_of(slot * 32, 32)

    def chunk_of(k):
        dy, dx = OFF[k]
        return ((y + dy) % 4) * 2 + (xh + dx) % 2

    loads = [
        pltpu.make_async_copy(phases, phases_v, small_sem.at[0]),
        pltpu.make_async_copy(bins, bins_v, small_sem.at[1]),
    ]
    inters, coefs = [], []
    for k in range(8):
        at = pl.ds(pl.multiple_of(chunk_of(k) * 512, 512), 512)
        inters.append(pltpu.make_async_copy(interp.at[at, :], interp_v.at[k], in_sem.at[k]))
        coefs.append(pltpu.make_async_copy(coeffs.at[:, at], coeffs_v.at[:, pl.ds(512 * k, 512)], co_sem.at[k]))
    table = pltpu.make_async_copy(tables.at[slot // 4], table_v, small_sem.at[2])

    partners = [(x + 2 * dx, y + dy, z, c) for dy, dx in OFF[:7]]
    partners += [(x, y, z + dz, c + dc) for dz in range(4) for dc in range(2) if dz or dc]
    partners += [(x + 1 - 2 * xl, y, z, c)]
    partners += [(3 - x, y + dy, z, c) for dy in range(4)]
    barrier = pltpu.get_barrier_semaphore()
    for partner in partners:
        pl.semaphore_signal(barrier, inc=1, device_id=device(*partner), device_id_type=MESH)
    for load in [*loads, *inters, *coefs[:2]]:
        load.start()

    for load in loads:
        load.wait()
    ph = phases_v[...]
    hi = ph.astype(BF)
    phl_v[0:64, :] = hi
    phl_v[64:128, :] = (ph - hi.astype(F32)).astype(BF)

    def send(src, dst, ssem, rsem, to):
        return pltpu.make_async_remote_copy(
            src_ref=src, dst_ref=dst, send_sem=ssem, recv_sem=rsem, device_id=device(*to), device_id_type=MESH
        )

    def piece(k, q):
        dy, dx = OFF[k]
        n = 512 // NQ[k]
        at = pl.ds(q * n, n)
        cols = pl.ds(pl.multiple_of(rad * 256, 256), 256)
        i = BASE[k] + q
        return send(proj_v.at[pl.ds(512 * k + q * n, n), :], recv_v.at[at, cols], ps_sem.at[i], pr_sem.at[i], (x + 2 * dx, y + dy, z, c))

    for k in range(8):
        inters[k].wait()
        if k < 6:
            coefs[k + 2].start()
        elif k == 6:
            table.start()
        at = pl.ds(pl.multiple_of(chunk_of(k) * 512, 512), 512)
        which = bins_v[at][None, :]
        hot = ((lax.broadcasted_iota(jnp.int32, (128, 512), 0) & 63) == which).astype(F32).astype(BF)
        lifted = lax.dot_general(hot, phl_v[...], (((0,), (0,)), ((), ())), preferred_element_type=F32)
        proj_v[512 * k : 512 * k + 512, :] = (interp_v[k].astype(F32) * lifted).astype(BF)
        if k == 0:
            pl.semaphore_wait(barrier, len(partners))
        if k < 7:
            for q in range(FIRST[k]):
                piece(k, q).start()
        else:
            recv_v[:, pl.ds(pl.multiple_of(rad * 256, 256), 256)] = proj_v[3584:4096, :]

    for h in range(2):
        for k in range(4 * h, 4 * h + 4):
            coefs[k].wait()
        at = slice(2048 * h, 2048 * h + 2048)
        got = jnp.dot(coeffs_v[:, at], proj_v[at, :], preferred_element_type=F32)
        if h == 0:
            acc_v[...] = got
        else:
            part_v[...] = (acc_v[...] + got).astype(BF).T
    zc = [(dz, dc) for dz in (2, 1, 3, 0) for dc in (0, 1) if dz or dc]
    sums = []
    for i, (dz, dc) in enumerate(zc):
        to_slot = ((z + dz) % 4) * 2 + (c + dc) % 2
        src = part_v.at[pl.ds(pl.multiple_of(to_slot * 32, 32), 32), :]
        sums.append(send(src, rs_v.at[i], rss_sem.at[i], rsr_sem.at[i], (x, y, z + dz, c + dc)))
        sums[-1].start()
    a = lax.broadcasted_iota(jnp.int32, (480, 512), 0)
    b = lax.broadcasted_iota(jnp.int32, (480, 512), 1)
    low = b & 63
    perm_v[...] = jnp.where(low < 60, (a == (b >> 6) * 60 + low).astype(F32), 0.0).astype(BF)
    total = part_v[pl.ds(rows, 32), :].astype(F32)
    for i in range(7):
        sums[i].wait_recv()
        total = total + rs_v[i].astype(F32)
    xs_v[...] = total.astype(BF)
    pair = send(xs_v, xr_v, xx_sem.at[0], xx_sem.at[1], (x + 1 - 2 * xl, y, z, c))
    pair.start()
    for k, q in SECOND:
        piece(k, q).start()
    table.wait()
    pair.wait_recv()
    nodes = (xs_v[...].astype(F32) + xr_v[...].astype(F32)).astype(BF)
    turned = jnp.dot(nodes, table_v[...], preferred_element_type=F32).astype(BF)
    ang_v[y, xh, pl.ds(rows, 32), :] = jnp.dot(turned, perm_v[...], preferred_element_type=F32).astype(BF)

    def rows_of(i, dz):
        flip, dy = PLANE[i]
        at = pl.multiple_of((((z + dz) % 4) * 2 + c) * 32, 32)
        return ang_v.at[(y - dy) % 4, (xh + flip) % 2, pl.ds(at, 32), :]

    started = []

    def go(copy):
        copy.start()
        started.append(copy)

    def across(i):
        flip, dy = PLANE[i]
        to = (3 - x if flip else x, y + dy, z, c)
        return send(rows_of(0, 0), rows_of(0, 0), pls_sem.at[i], plr_sem.at[i], to)

    def along(i, step):
        n = 3 * i + (0 if step > 0 else 1)
        return send(rows_of(i, 0), rows_of(i, 0), zs_sem.at[n], zr_sem.at[n], (x, y, z + step, c))

    def relay(i):
        step = 1 if i % 2 else -1
        n = 3 * i + 2
        return send(rows_of(i, -step), rows_of(i, -step), zs_sem.at[n], zr_sem.at[n], (x, y, z + step, c))

    def other_core(i, dz):
        n = 4 * i + dz % 4
        return send(rows_of(i, dz), rows_of(i, dz), cs_sem.at[n], cr_sem.at[n], (x, y, z, c + 1))

    def near(i):
        step = 1 if i % 2 else -1
        along(i, step).wait_recv()
        go(relay(i))
        go(other_core(i, -step))
        along(i, -step).wait_recv()
        go(other_core(i, step))

    for i in (7, 4, 5, 6, 1, 2, 3):
        go(across(i))
    for i in range(8):
        if i:
            across(i).wait_recv()
        go(along(i, 1))
        go(along(i, -1))
        go(other_core(i, 0))
        for k, q in THIRD.get(i, ()):
            piece(k, q).start()
        if i >= LAG:
            near(i - LAG)
    for i in range(8 - LAG, 8):
        near(i)
    for i in range(8):
        relay(i).wait_recv()
        go(other_core(i, 2))
    for i in range(8):
        for dz in range(4):
            other_core(i, dz).wait_recv()

    for k in range(7):
        for q in range(NQ[k]):
            piece(k, q).wait_recv()
    sent = {}
    for b in range(2):
        dys = ((2, 1), (3, 0))[b]
        cols = [ang_v[:, :, :, pl.ds(pl.multiple_of(((y + dy) % 4) * 128, 128), 128)].reshape(2048, 128) for dy in dys]
        res = jnp.dot(recv_v[...], jnp.concatenate(cols, axis=1), preferred_element_type=F32)
        fsend_v[4 * b : 4 * b + 4] = res.astype(BF).T.reshape(4, 64, 512)
        for k in range(4 * b, min(4 * b + 4, 7)):
            dy, dx = OFF[k]
            src = fsend_v.at[k // 2 * 2 + (xh + dx) % 2]
            sent[k] = send(src, frecv_v.at[k], fs_sem.at[k], fr_sem.at[k], (x + 2 * dx, y + dy, z, c))
            sent[k].start()
    outs = []
    for k in (7, 6, 5, 3, 4, 2, 1, 0):
        dy, dx = OFF[k]
        if k < 7:
            sent[k].wait_recv()
            block = frecv_v[k]
        else:
            block = fsend_v[6 + xh]
        source = ((y - dy) % 4) * 2 + (xh + dx) % 2
        at = pl.multiple_of(source * 512, 512)
        out[:, pl.ds(at, 512)] = block[:60, :]

    for k in range(7):
        for q in range(NQ[k]):
            piece(k, q).wait_send()
        sums[k].wait_send()
        sent[k].wait_send()
    pair.wait_send()
    for copy in started:
        copy.wait_send()


def body(coeffs, interp, phases, tables, bins):
    dma = pltpu.SemaphoreType.DMA
    return pl.pallas_call(
        kernel,
        name="coupling",
        out_shape=pltpu.VMEM((60, 4096), BF),
        in_specs=[pl.BlockSpec(memory_space=pl.ANY)] * 5,
        out_specs=pl.BlockSpec(memory_space=pltpu.VMEM),
        scratch_shapes=[
            pltpu.VMEM((8, 512, 256), BF),
            pltpu.VMEM((480, 4096), BF),
            pltpu.VMEM((64, 256), F32),
            pltpu.VMEM((4096,), jnp.int32),
            pltpu.VMEM((480, 480), BF),
            pltpu.VMEM((128, 256), BF),
            pltpu.VMEM((480, 512), BF),
            pltpu.VMEM((4096, 256), BF),
            pltpu.VMEM((512, 2048), BF),
            pltpu.VMEM((480, 256), F32),
            pltpu.VMEM((256, 480), BF),
            pltpu.VMEM((7, 32, 480), BF),
            pltpu.VMEM((32, 480), BF),
            pltpu.VMEM((32, 480), BF),
            pltpu.VMEM((4, 2, 256, 512), BF),
            pltpu.VMEM((8, 64, 512), BF),
            pltpu.VMEM((7, 64, 512), BF),
            pltpu.VMEM((60, 4096), BF),
            dma((8,)), dma((8,)), dma((3,)), dma((NPIECE,)), dma((NPIECE,)), dma((7,)), dma((7,)), dma((2,)),
            dma((8,)), dma((8,)), dma((24,)), dma((24,)), dma((32,)), dma((32,)), dma((7,)), dma((7,)), dma((8,)),
        ],
        compiler_params=pltpu.CompilerParams(
            collective_id=0, has_side_effects=True, vmem_limit_bytes=60 * 1024 * 1024
        ),
    )(coeffs.T, interp, phases, tables, bins).T


def solution(mesh):
    return jax.shard_map(
        body,
        mesh=mesh,
        in_specs=(P("sph", None), P("sph", "rad"), P(None, "rad"), P("rad", None, None), P("sph")),
        out_specs=P("sph", "rad"),
        check_vma=False,
    )
```

```python
import functools

import jax
import jax.numpy as jnp
from jax import lax
from jax.experimental import pallas as pl
from jax.experimental.pallas import tpu as pltpu
from jax.sharding import PartitionSpec as P

MESH = pl.DeviceIdType.MESH
BF = jnp.bfloat16
F32 = jnp.float32

OFF = [(2, 1), (2, 0), (1, 1), (1, 0), (3, 1), (3, 0), (0, 1), (0, 0)]
XK = [k for k, (dy, dx) in enumerate(OFF) if dx]
NQ = [4 if dx else 2 for dy, dx in OFF[:7]]
BASE = [sum(NQ[:k]) for k in range(7)]
NPIECE = sum(NQ)
FIRST = {0: 2, 1: 1, 2: 2, 3: 1, 4: 1, 5: 1, 6: 1}
SECOND = [(6, 1)]
REST = [(4, 1), (0, 2), (2, 2), (1, 1), (4, 2), (6, 2), (3, 1), (0, 3), (2, 3), (5, 1), (4, 3), (6, 3)]
THIRD = {3: REST[:3], 7: REST[3:]}
PLANE = [(0, 0), (0, 1), (0, 3), (1, 0), (0, 2), (1, 1), (1, 3), (1, 2)]
LAG = 8
GROUP = 4


def where():
    s, r = lax.axis_index("sph"), lax.axis_index("rad")
    return (r % 2) * 2 + s // 8, r // 2, (s // 2) % 4, s % 2


def device(x, y, z, c):
    x, y, z, c = x % 4, y % 4, z % 4, c % 2
    return (x % 2) * 8 + z * 2 + c, y * 2 + x // 2


def kernel(
    coeffs, interp, phases, tables, bins, out,
    interp_v, coeffs_v, phases_v, bins_v, table_v, phl_v, perm_v, proj_v, recv_v, acc_v, part_v,
    rs_v, xs_v, xr_v, ang_v, fsend_v, frecv_v,
    in_sem, co_sem, small_sem, ps_sem, pr_sem, rss_sem, rsr_sem, xx_sem, pls_sem, plr_sem,
    zs_sem, zr_sem, cs_sem, cr_sem, fs_sem, fr_sem,
):
    x, y, z, c = where()
    xh, xl = x // 2, x % 2
    rad, slot = y * 2 + xh, z * 2 + c
    rows = pl.multiple_of(slot * 32, 32)

    def chunk_of(k):
        dy, dx = OFF[k]
        return ((y + dy) % 4) * 2 + (xh + dx) % 2

    loads = [
        pltpu.make_async_copy(phases, phases_v, small_sem.at[0]),
        pltpu.make_async_copy(bins, bins_v, small_sem.at[1]),
    ]
    inters, coefs = [], []
    for k in range(8):
        at = pl.ds(pl.multiple_of(chunk_of(k) * 512, 512), 512)
        inters.append(pltpu.make_async_copy(interp.at[at, :], interp_v.at[k], in_sem.at[k]))
        coefs.append(pltpu.make_async_copy(coeffs.at[:, at], coeffs_v.at[:, pl.ds(512 * k, 512)], co_sem.at[k]))
    table = pltpu.make_async_copy(tables.at[slot // 4], table_v, small_sem.at[2])

    partners = [(x + 2 * dx, y + dy, z, c) for dy, dx in OFF[:7]]
    partners += [(x, y, z + dz, c + dc) for dz in range(4) for dc in range(2) if dz or dc]
    partners += [(x + 1 - 2 * xl, y, z, c)]
    partners += [(3 - x, y + dy, z, c) for dy in range(4)]
    barrier = pltpu.get_barrier_semaphore()
    for partner in partners:
        pl.semaphore_signal(barrier, inc=1, device_id=device(*partner), device_id_type=MESH)
    for load in loads:
        load.start()

    for load in [*inters, *coefs[:2]]:
        load.start()
    for load in loads:
        load.wait()
    ph = phases_v[...]
    hi = ph.astype(BF)
    phl_v[0:64, :] = hi
    phl_v[64:128, :] = (ph - hi.astype(F32)).astype(BF)

    def send(src, dst, ssem, rsem, to):
        return pltpu.make_async_remote_copy(
            src_ref=src, dst_ref=dst, send_sem=ssem, recv_sem=rsem, device_id=device(*to), device_id_type=MESH
        )

    def piece(k, q):
        dy, dx = OFF[k]
        n = 512 // NQ[k]
        at = pl.ds(q * n, n)
        cols = pl.ds(pl.multiple_of(rad * 256, 256), 256)
        i = BASE[k] + q
        return send(proj_v.at[pl.ds(512 * k + q * n, n), :], recv_v.at[at, cols], ps_sem.at[i], pr_sem.at[i], (x + 2 * dx, y + dy, z, c))

    for k0 in range(0, 8, GROUP):
        ks = range(k0, k0 + GROUP)
        for k in ks:
            inters[k].wait()
        for k in ks:
            at = pl.ds(pl.multiple_of(chunk_of(k) * 512, 512), 512)
            which = bins_v[at][None, :]
            hot = ((lax.broadcasted_iota(jnp.int32, (128, 512), 0) & 63) == which).astype(F32).astype(BF)
            lifted = lax.dot_general(hot, phl_v[...], (((0,), (0,)), ((), ())), preferred_element_type=F32)
            proj_v[512 * k : 512 * k + 512, :] = (interp_v[k].astype(F32) * lifted).astype(BF)
        if k0 == 0:
            for k in range(2, 8):
                coefs[k].start()
            table.start()
            pl.semaphore_wait(barrier, len(partners))
        for k in ks:
            if k < 7:
                for q in range(FIRST[k]):
                    piece(k, q).start()
    recv_v[:, pl.ds(pl.multiple_of(rad * 256, 256), 256)] = proj_v[3584:4096, :]

    for k in range(8):
        coefs[k].wait()
    part_v[...] = lax.dot_general(proj_v[...], coeffs_v[...], (((0,), (1,)), ((), ())), preferred_element_type=F32).astype(BF)
    zc = [(dz, dc) for dz in (2, 1, 3, 0) for dc in (0, 1) if dz or dc]
    sums = []
    for i, (dz, dc) in enumerate(zc):
        to_slot = ((z + dz) % 4) * 2 + (c + dc) % 2
        src = part_v.at[pl.ds(pl.multiple_of(to_slot * 32, 32), 32), :]
        sums.append(send(src, rs_v.at[i], rss_sem.at[i], rsr_sem.at[i], (x, y, z + dz, c + dc)))
        sums[-1].start()
    a = lax.broadcasted_iota(jnp.int32, (480, 512), 0)
    b = lax.broadcasted_iota(jnp.int32, (480, 512), 1)
    low = b & 63
    perm_v[...] = jnp.where(low < 60, (a == (b >> 6) * 60 + low).astype(F32), 0.0).astype(BF)
    total = part_v[pl.ds(rows, 32), :].astype(F32)
    for i in range(7):
        sums[i].wait_recv()
        total = total + rs_v[i].astype(F32)
    xs_v[...] = total.astype(BF)
    pair = send(xs_v, xr_v, xx_sem.at[0], xx_sem.at[1], (x + 1 - 2 * xl, y, z, c))
    pair.start()
    for k, q in SECOND:
        piece(k, q).start()
    table.wait()
    pair.wait_recv()
    nodes = (xs_v[...].astype(F32) + xr_v[...].astype(F32)).astype(BF)
    turned = jnp.dot(nodes, table_v[...], preferred_element_type=F32).astype(BF)
    ang_v[y, xh, pl.ds(rows, 32), :] = jnp.dot(turned, perm_v[...], preferred_element_type=F32).astype(BF)

    def rows_of(i, dz):
        flip, dy = PLANE[i]
        at = pl.multiple_of((((z + dz) % 4) * 2 + c) * 32, 32)
        return ang_v.at[(y - dy) % 4, (xh + flip) % 2, pl.ds(at, 32), :]

    started = []

    def go(copy):
        copy.start()
        started.append(copy)

    def across(i):
        flip, dy = PLANE[i]
        to = (3 - x if flip else x, y + dy, z, c)
        return send(rows_of(0, 0), rows_of(0, 0), pls_sem.at[i], plr_sem.at[i], to)

    def along(i, step):
        n = 3 * i + (0 if step > 0 else 1)
        return send(rows_of(i, 0), rows_of(i, 0), zs_sem.at[n], zr_sem.at[n], (x, y, z + step, c))

    def relay(i):
        step = 1 if i % 2 else -1
        n = 3 * i + 2
        return send(rows_of(i, -step), rows_of(i, -step), zs_sem.at[n], zr_sem.at[n], (x, y, z + step, c))

    def other_core(i, dz):
        n = 4 * i + dz % 4
        return send(rows_of(i, dz), rows_of(i, dz), cs_sem.at[n], cr_sem.at[n], (x, y, z, c + 1))

    def near(i):
        step = 1 if i % 2 else -1
        along(i, step).wait_recv()
        go(relay(i))
        go(other_core(i, -step))
        along(i, -step).wait_recv()
        go(other_core(i, step))

    for i in (7, 4, 5, 6, 1, 2, 3):
        go(across(i))
    for i in range(8):
        if i:
            across(i).wait_recv()
        go(along(i, 1))
        go(along(i, -1))
        go(other_core(i, 0))
        for k, q in THIRD.get(i, ()):
            piece(k, q).start()
        if i >= LAG:
            near(i - LAG)
    for i in range(8 - LAG, 8):
        near(i)
    for i in range(8):
        relay(i).wait_recv()
        go(other_core(i, 2))
    for i in range(8):
        for dz in range(4):
            other_core(i, dz).wait_recv()

    def back(k, h):
        dy, dx = OFF[k]
        half = slice(256 * h, 256 * h + 256)
        src = fsend_v.at[k // 2 * 2 + (xh + dx) % 2, :, half]
        to = (x + 2 * dx, y + dy, z, c)
        return send(src, frecv_v.at[k, :, half], fs_sem.at[2 * k + h], fr_sem.at[2 * k + h], to)

    for h in range(2):
        for k in range(7):
            for q in range(NQ[k] // 2 * h, NQ[k] // 2 * (h + 1)):
                piece(k, q).wait_recv()
        cols = [ang_v[:, :, :, pl.ds(pl.multiple_of(((y + dy) % 4) * 128, 128), 128)] for dy in (2, 1, 3, 0)]
        cols = jnp.concatenate([part.reshape(2048, 128) for part in cols], axis=1)
        res = jnp.dot(recv_v[256 * h : 256 * h + 256, :], cols, preferred_element_type=F32)
        fsend_v[:, :, 256 * h : 256 * h + 256] = res.astype(BF).T.reshape(8, 64, 256)
        for k in range(7):
            back(k, h).start()
    for h in range(2):
        for k in (7, 6, 5, 3, 4, 2, 1, 0):
            dy, dx = OFF[k]
            half = slice(256 * h, 256 * h + 256)
            if k < 7:
                back(k, h).wait_recv()
                block = frecv_v[k, :, half]
            else:
                block = fsend_v[6 + xh, :, half]
            source = ((y - dy) % 4) * 2 + (xh + dx) % 2
            out[:, pl.ds(pl.multiple_of(source * 512 + 256 * h, 256), 256)] = block[:60, :]

    for k in range(7):
        for q in range(NQ[k]):
            piece(k, q).wait_send()
        sums[k].wait_send()
        back(k, 0).wait_send()
        back(k, 1).wait_send()
    pair.wait_send()
    for copy in started:
        copy.wait_send()


def body(coeffs, interp, phases, tables, bins):
    dma = pltpu.SemaphoreType.DMA
    return pl.pallas_call(
        kernel,
        name="coupling",
        out_shape=pltpu.VMEM((60, 4096), BF),
        in_specs=[pl.BlockSpec(memory_space=pl.ANY)] * 5,
        out_specs=pl.BlockSpec(memory_space=pltpu.VMEM),
        scratch_shapes=[
            pltpu.VMEM((8, 512, 256), BF),
            pltpu.VMEM((480, 4096), BF),
            pltpu.VMEM((64, 256), F32),
            pltpu.VMEM((4096,), jnp.int32),
            pltpu.VMEM((480, 480), BF),
            pltpu.VMEM((128, 256), BF),
            pltpu.VMEM((480, 512), BF),
            pltpu.VMEM((4096, 256), BF),
            pltpu.VMEM((512, 2048), BF),
            pltpu.VMEM((480, 256), F32),
            pltpu.VMEM((256, 480), BF),
            pltpu.VMEM((7, 32, 480), BF),
            pltpu.VMEM((32, 480), BF),
            pltpu.VMEM((32, 480), BF),
            pltpu.VMEM((4, 2, 256, 512), BF),
            pltpu.VMEM((8, 64, 512), BF),
            pltpu.VMEM((7, 64, 512), BF),
            dma((8,)), dma((8,)), dma((3,)), dma((NPIECE,)), dma((NPIECE,)), dma((7,)), dma((7,)), dma((2,)),
            dma((8,)), dma((8,)), dma((24,)), dma((24,)), dma((32,)), dma((32,)), dma((14,)), dma((14,)),
        ],
        compiler_params=pltpu.CompilerParams(
            collective_id=0, has_side_effects=True, vmem_limit_bytes=60 * 1024 * 1024
        ),
    )(coeffs.T, interp, phases, tables, bins).T


def solution(mesh):
    return jax.shard_map(
        body,
        mesh=mesh,
        in_specs=(P("sph", None), P("sph", "rad"), P(None, "rad"), P("rad", None, None), P("sph")),
        out_specs=P("sph", "rad"),
        check_vma=False,
    )
```

```python
import functools

import jax
import jax.numpy as jnp
from jax import lax
from jax.experimental import pallas as pl
from jax.experimental.pallas import tpu as pltpu
from jax.sharding import PartitionSpec as P

MESH = pl.DeviceIdType.MESH
BF = jnp.bfloat16
F32 = jnp.float32

OFF = [(2, 1), (2, 0), (1, 1), (1, 0), (3, 1), (3, 0), (0, 1), (0, 0)]
XK = [k for k, (dy, dx) in enumerate(OFF) if dx]
NQ = [4 if dx else 2 for dy, dx in OFF[:7]]
BASE = [sum(NQ[:k]) for k in range(7)]
NPIECE = sum(NQ)
FIRST = {0: 2, 1: 1, 2: 2, 3: 1, 4: 1, 5: 1, 6: 1}
SECOND = [(6, 1)]
REST = [(4, 1), (0, 2), (2, 2), (1, 1), (4, 2), (6, 2), (0, 3), (2, 3), (4, 3), (6, 3)]
THIRD = {3: REST[:3], 7: REST[3:]}
PLANE = [(0, 0), (0, 1), (0, 3), (1, 0), (0, 2), (1, 1), (1, 3), (1, 2)]
LAG = 8
EARLY = [(3, 1), (5, 1)]
EXTRA = []
GROUP = 4


def where():
    s, r = lax.axis_index("sph"), lax.axis_index("rad")
    return (r % 2) * 2 + s // 8, r // 2, (s // 2) % 4, s % 2


def device(x, y, z, c):
    x, y, z, c = x % 4, y % 4, z % 4, c % 2
    return (x % 2) * 8 + z * 2 + c, y * 2 + x // 2


def kernel(
    coeffs, interp, phases, tables, bins, out,
    interp_v, coeffs_v, phases_v, bins_v, table_v, phl_v, perm_v, proj_v, recv_v, acc_v, part_v,
    rs_v, xs_v, xr_v, ang_v, fsend_v, frecv_v,
    in_sem, co_sem, small_sem, ps_sem, pr_sem, rss_sem, rsr_sem, xx_sem, pls_sem, plr_sem,
    zs_sem, zr_sem, cs_sem, cr_sem, fs_sem, fr_sem, later,
):
    x, y, z, c = where()
    xh, xl = x // 2, x % 2
    rad, slot = y * 2 + xh, z * 2 + c
    rows = pl.multiple_of(slot * 32, 32)

    def chunk_of(k):
        dy, dx = OFF[k]
        return ((y + dy) % 4) * 2 + (xh + dx) % 2

    loads = [
        pltpu.make_async_copy(phases, phases_v, small_sem.at[0]),
        pltpu.make_async_copy(bins, bins_v, small_sem.at[1]),
    ]
    inters, coefs = [], []
    for k in range(8):
        at = pl.ds(pl.multiple_of(chunk_of(k) * 512, 512), 512)
        inters.append(pltpu.make_async_copy(interp.at[at, :], interp_v.at[k], in_sem.at[k]))
        coefs.append(pltpu.make_async_copy(coeffs.at[:, at], coeffs_v.at[:, pl.ds(512 * k, 512)], co_sem.at[k]))
    table = pltpu.make_async_copy(tables.at[slot // 4], table_v, small_sem.at[2])

    partners = [(x + 2 * dx, y + dy, z, c) for dy, dx in OFF[:7]]
    partners += [(x, y, z, c + 1), (x + 1 - 2 * xl, y, z, c)]
    partners += [(3 - x, y + dy, z, c) for dy in range(4)]
    barrier = pltpu.get_barrier_semaphore()
    for partner in partners:
        pl.semaphore_signal(barrier, inc=1, device_id=device(*partner), device_id_type=MESH)
    for dz in range(1, 4):

        @pl.when(z + dz < 4)
        def _():
            for dc in range(2):
                pl.semaphore_signal(barrier, inc=1, device_id=device(x, y, z + dz, c + dc), device_id_type=MESH)

    for load in loads:
        load.start()

    for load in [*inters, *coefs[:2]]:
        load.start()
    for load in loads:
        load.wait()
    ph = phases_v[...]
    hi = ph.astype(BF)
    phl_v[0:64, :] = hi
    phl_v[64:128, :] = (ph - hi.astype(F32)).astype(BF)

    def send(src, dst, ssem, rsem, to):
        return pltpu.make_async_remote_copy(
            src_ref=src, dst_ref=dst, send_sem=ssem, recv_sem=rsem, device_id=device(*to), device_id_type=MESH
        )

    def piece(k, q):
        dy, dx = OFF[k]
        n = 512 // NQ[k]
        at = pl.ds(q * n, n)
        cols = pl.ds(pl.multiple_of(rad * 256, 256), 256)
        i = BASE[k] + q
        return send(proj_v.at[pl.ds(512 * k + q * n, n), :], recv_v.at[at, cols], ps_sem.at[i], pr_sem.at[i], (x + 2 * dx, y + dy, z, c))

    for k0 in range(0, 8, GROUP):
        ks = range(k0, k0 + GROUP)
        for k in ks:
            inters[k].wait()
        for k in ks:
            at = pl.ds(pl.multiple_of(chunk_of(k) * 512, 512), 512)
            which = bins_v[at][None, :]
            hot = ((lax.broadcasted_iota(jnp.int32, (128, 512), 0) & 63) == which).astype(F32).astype(BF)
            lifted = lax.dot_general(hot, phl_v[...], (((0,), (0,)), ((), ())), preferred_element_type=F32)
            proj_v[512 * k : 512 * k + 512, :] = (interp_v[k].astype(F32) * lifted).astype(BF)
        if k0 == 0:
            for k in range(2, 8):
                coefs[k].start()
            table.start()
            pl.semaphore_wait(barrier, len(partners) + 2 * z)
            for dz in range(1, 4):

                @pl.when(z + dz >= 4)
                def _():
                    for dc in range(2):
                        pl.semaphore_signal(later, inc=1, device_id=device(x, y, z + dz, c + dc), device_id_type=MESH)

        for k in ks:
            if k < 7:
                for q in range(FIRST[k]):
                    piece(k, q).start()
    for (k, q), last in EXTRA:
        pl.when(z <= last)(piece(k, q).start)
    recv_v[:, pl.ds(pl.multiple_of(rad * 256, 256), 256)] = proj_v[3584:4096, :]

    for k in range(8):
        coefs[k].wait()
    part_v[...] = lax.dot_general(proj_v[...], coeffs_v[...], (((0,), (1,)), ((), ())), preferred_element_type=F32).astype(BF)

    @pl.when(z < 3)
    def _():
        pl.semaphore_wait(later, 6 - 2 * z)

    zc = [(dz, dc) for dz in (2, 1, 3, 0) for dc in (0, 1) if dz or dc]
    sums = []
    for i, (dz, dc) in enumerate(zc):
        to_slot = ((z + dz) % 4) * 2 + (c + dc) % 2
        src = part_v.at[pl.ds(pl.multiple_of(to_slot * 32, 32), 32), :]
        sums.append(send(src, rs_v.at[i], rss_sem.at[i], rsr_sem.at[i], (x, y, z + dz, c + dc)))
        sums[-1].start()
    a = lax.broadcasted_iota(jnp.int32, (480, 512), 0)
    b = lax.broadcasted_iota(jnp.int32, (480, 512), 1)
    low = b & 63
    perm_v[...] = jnp.where(low < 60, (a == (b >> 6) * 60 + low).astype(F32), 0.0).astype(BF)
    total = part_v[pl.ds(rows, 32), :].astype(F32)
    for i in range(7):
        sums[i].wait_recv()
        total = total + rs_v[i].astype(F32)
    xs_v[...] = total.astype(BF)
    pair = send(xs_v, xr_v, xx_sem.at[0], xx_sem.at[1], (x + 1 - 2 * xl, y, z, c))
    pair.start()
    for k, q in SECOND:
        piece(k, q).start()
    table.wait()
    pair.wait_recv()
    nodes = (xs_v[...].astype(F32) + xr_v[...].astype(F32)).astype(BF)
    turned = jnp.dot(nodes, table_v[...], preferred_element_type=F32).astype(BF)
    ang_v[y, xh, pl.ds(rows, 32), :] = jnp.dot(turned, perm_v[...], preferred_element_type=F32).astype(BF)

    def rows_of(i, dz):
        flip, dy = PLANE[i]
        at = pl.multiple_of((((z + dz) % 4) * 2 + c) * 32, 32)
        return ang_v.at[(y - dy) % 4, (xh + flip) % 2, pl.ds(at, 32), :]

    started = []

    def go(copy):
        copy.start()
        started.append(copy)

    def across(i):
        flip, dy = PLANE[i]
        to = (3 - x if flip else x, y + dy, z, c)
        return send(rows_of(0, 0), rows_of(0, 0), pls_sem.at[i], plr_sem.at[i], to)

    def along(i, step):
        n = 3 * i + (0 if step > 0 else 1)
        return send(rows_of(i, 0), rows_of(i, 0), zs_sem.at[n], zr_sem.at[n], (x, y, z + step, c))

    def relay(i):
        step = 1 if i % 2 else -1
        n = 3 * i + 2
        return send(rows_of(i, -step), rows_of(i, -step), zs_sem.at[n], zr_sem.at[n], (x, y, z + step, c))

    def other_core(i, dz):
        n = 4 * i + dz % 4
        return send(rows_of(i, dz), rows_of(i, dz), cs_sem.at[n], cr_sem.at[n], (x, y, z, c + 1))

    def near(i):
        step = 1 if i % 2 else -1
        along(i, step).wait_recv()
        go(relay(i))
        go(other_core(i, -step))
        along(i, -step).wait_recv()
        go(other_core(i, step))

    for i in (7, 4, 5, 6, 1, 2, 3):
        across(i).start()
    for step in (1, -1):
        go(along(0, step))
    go(other_core(0, 0))
    for i in (7, 4, 5, 6, 1, 2, 3):
        across(i).wait_send()
    for k, q in EARLY:
        piece(k, q).start()
    for i in range(8):
        if i:
            across(i).wait_recv()
            go(along(i, 1))
            go(along(i, -1))
            go(other_core(i, 0))
        if i == 7:
            for (k, q), last in EXTRA:
                pl.when(z > last)(piece(k, q).start)
        for k, q in THIRD.get(i, ()):
            piece(k, q).start()
        if i >= LAG:
            near(i - LAG)
    for i in range(8 - LAG, 8):
        near(i)
    for i in range(8):
        relay(i).wait_recv()
        go(other_core(i, 2))
    for i in range(8):
        for dz in range(4):
            other_core(i, dz).wait_recv()

    def back(k, h):
        dy, dx = OFF[k]
        half = slice(256 * h, 256 * h + 256)
        src = fsend_v.at[k // 2 * 2 + (xh + dx) % 2, :, half]
        to = (x + 2 * dx, y + dy, z, c)
        return send(src, frecv_v.at[k, :, half], fs_sem.at[2 * k + h], fr_sem.at[2 * k + h], to)

    for h in range(2):
        for k in range(7):
            for q in range(NQ[k] // 2 * h, NQ[k] // 2 * (h + 1)):
                piece(k, q).wait_recv()
        cols = [ang_v[:, :, :, pl.ds(pl.multiple_of(((y + dy) % 4) * 128, 128), 128)] for dy in (2, 1, 3, 0)]
        cols = jnp.concatenate([part.reshape(2048, 128) for part in cols], axis=1)
        res = jnp.dot(recv_v[256 * h : 256 * h + 256, :], cols, preferred_element_type=F32)
        fsend_v[:, :, 256 * h : 256 * h + 256] = res.astype(BF).T.reshape(8, 64, 256)
        for k in range(7):
            back(k, h).start()
    for h in range(2):
        for k in (7, 6, 5, 3, 4, 2, 1, 0):
            dy, dx = OFF[k]
            half = slice(256 * h, 256 * h + 256)
            if k < 7:
                back(k, h).wait_recv()
                block = frecv_v[k, :, half]
            else:
                block = fsend_v[6 + xh, :, half]
            source = ((y - dy) % 4) * 2 + (xh + dx) % 2
            out[:, pl.ds(pl.multiple_of(source * 512 + 256 * h, 256), 256)] = block[:60, :]

    for k in range(7):
        for q in range(NQ[k]):
            piece(k, q).wait_send()
        sums[k].wait_send()
        back(k, 0).wait_send()
        back(k, 1).wait_send()
    pair.wait_send()
    for copy in started:
        copy.wait_send()


def body(coeffs, interp, phases, tables, bins):
    dma = pltpu.SemaphoreType.DMA
    return pl.pallas_call(
        kernel,
        name="coupling",
        out_shape=pltpu.VMEM((60, 4096), BF),
        in_specs=[pl.BlockSpec(memory_space=pl.ANY)] * 5,
        out_specs=pl.BlockSpec(memory_space=pltpu.VMEM),
        scratch_shapes=[
            pltpu.VMEM((8, 512, 256), BF),
            pltpu.VMEM((480, 4096), BF),
            pltpu.VMEM((64, 256), F32),
            pltpu.VMEM((4096,), jnp.int32),
            pltpu.VMEM((480, 480), BF),
            pltpu.VMEM((128, 256), BF),
            pltpu.VMEM((480, 512), BF),
            pltpu.VMEM((4096, 256), BF),
            pltpu.VMEM((512, 2048), BF),
            pltpu.VMEM((480, 256), F32),
            pltpu.VMEM((256, 480), BF),
            pltpu.VMEM((7, 32, 480), BF),
            pltpu.VMEM((32, 480), BF),
            pltpu.VMEM((32, 480), BF),
            pltpu.VMEM((4, 2, 256, 512), BF),
            pltpu.VMEM((8, 64, 512), BF),
            pltpu.VMEM((7, 64, 512), BF),
            dma((8,)), dma((8,)), dma((3,)), dma((NPIECE,)), dma((NPIECE,)), dma((7,)), dma((7,)), dma((2,)),
            dma((8,)), dma((8,)), dma((24,)), dma((24,)), dma((32,)), dma((32,)), dma((14,)), dma((14,)), pltpu.SemaphoreType.REGULAR,
        ],
        compiler_params=pltpu.CompilerParams(
            collective_id=0, has_side_effects=True, vmem_limit_bytes=60 * 1024 * 1024
        ),
    )(coeffs.T, interp, phases, tables, bins).T


def solution(mesh):
    return jax.shard_map(
        body,
        mesh=mesh,
        in_specs=(P("sph", None), P("sph", "rad"), P(None, "rad"), P("rad", None, None), P("sph")),
        out_specs=P("sph", "rad"),
        check_vma=False,
    )
```

```python
import functools

import jax
import jax.numpy as jnp
from jax import lax
from jax.experimental import pallas as pl
from jax.experimental.pallas import tpu as pltpu
from jax.sharding import PartitionSpec as P

MESH = pl.DeviceIdType.MESH
BF = jnp.bfloat16
F32 = jnp.float32

OFF = [(2, 1), (2, 0), (1, 1), (1, 0), (3, 1), (3, 0), (0, 1), (0, 0)]
XK = [k for k, (dy, dx) in enumerate(OFF) if dx]
NQ = [4 if dx else 2 for dy, dx in OFF[:7]]
BASE = [sum(NQ[:k]) for k in range(7)]
NPIECE = sum(NQ)
FIRST = {0: 2, 1: 1, 2: 2, 3: 1, 4: 1, 5: 1, 6: 1}
SECOND = [(6, 1)]
REST = [(4, 1), (0, 2), (2, 2), (1, 1), (4, 2), (0, 3), (2, 3), (4, 3), (6, 3)]
THIRD = {7: REST}
PLANE = [(0, 0), (0, 1), (0, 3), (1, 0), (0, 2), (1, 1), (1, 3), (1, 2)]
LAG = 8
EARLY = [(3, 1), (5, 1)]
EXTRA = [((6, 2), 0)]
GROUP = 2


def where():
    s, r = lax.axis_index("sph"), lax.axis_index("rad")
    return (r % 2) * 2 + s // 8, r // 2, (s // 2) % 4, s % 2


def device(x, y, z, c):
    x, y, z, c = x % 4, y % 4, z % 4, c % 2
    return (x % 2) * 8 + z * 2 + c, y * 2 + x // 2


def kernel(
    coeffs, interp, phases, tables, bins, out,
    interp_v, coeffs_v, phases_v, bins_v, table_v, phl_v, perm_v, proj_v, recv_v, acc_v, part_v,
    rs_v, xs_v, xr_v, ang_v, fsend_v, frecv_v,
    in_sem, co_sem, small_sem, ps_sem, pr_sem, rss_sem, rsr_sem, xx_sem, pls_sem, plr_sem,
    zs_sem, zr_sem, cs_sem, cr_sem, fs_sem, fr_sem, later,
):
    x, y, z, c = where()
    xh, xl = x // 2, x % 2
    rad, slot = y * 2 + xh, z * 2 + c
    rows = pl.multiple_of(slot * 32, 32)

    def chunk_of(k):
        dy, dx = OFF[k]
        return ((y + dy) % 4) * 2 + (xh + dx) % 2

    loads = [
        pltpu.make_async_copy(phases, phases_v, small_sem.at[0]),
        pltpu.make_async_copy(bins, bins_v, small_sem.at[1]),
    ]
    inters, coefs = [], []
    for k in range(8):
        at = pl.ds(pl.multiple_of(chunk_of(k) * 512, 512), 512)
        inters.append(pltpu.make_async_copy(interp.at[at, :], interp_v.at[k], in_sem.at[k]))
        coefs.append(pltpu.make_async_copy(coeffs.at[:, at], coeffs_v.at[:, pl.ds(512 * k, 512)], co_sem.at[k]))
    table = pltpu.make_async_copy(tables.at[slot // 4], table_v, small_sem.at[2])

    partners = [(x + 2 * dx, y + dy, z, c) for dy, dx in OFF[:7]]
    partners += [(x, y, z, c + 1), (x + 1 - 2 * xl, y, z, c)]
    partners += [(3 - x, y + dy, z, c) for dy in range(4)]
    barrier = pltpu.get_barrier_semaphore()
    for partner in partners:
        pl.semaphore_signal(barrier, inc=1, device_id=device(*partner), device_id_type=MESH)
    for dz in range(1, 4):

        @pl.when(z + dz < 4)
        def _():
            for dc in range(2):
                pl.semaphore_signal(barrier, inc=1, device_id=device(x, y, z + dz, c + dc), device_id_type=MESH)

    for load in loads:
        load.start()

    for load in [*inters, *coefs[:2]]:
        load.start()
    for load in loads:
        load.wait()
    ph = phases_v[...]
    hi = ph.astype(BF)
    phl_v[0:64, :] = hi
    phl_v[64:128, :] = (ph - hi.astype(F32)).astype(BF)

    def send(src, dst, ssem, rsem, to):
        return pltpu.make_async_remote_copy(
            src_ref=src, dst_ref=dst, send_sem=ssem, recv_sem=rsem, device_id=device(*to), device_id_type=MESH
        )

    def piece(k, q):
        dy, dx = OFF[k]
        n = 512 // NQ[k]
        at = pl.ds(q * n, n)
        cols = pl.ds(pl.multiple_of(rad * 256, 256), 256)
        i = BASE[k] + q
        return send(proj_v.at[pl.ds(512 * k + q * n, n), :], recv_v.at[at, cols], ps_sem.at[i], pr_sem.at[i], (x + 2 * dx, y + dy, z, c))

    for k0 in range(0, 8, GROUP):
        ks = range(k0, k0 + GROUP)
        for k in ks:
            inters[k].wait()
        for k in ks:
            at = pl.ds(pl.multiple_of(chunk_of(k) * 512, 512), 512)
            which = bins_v[at][None, :]
            hot = ((lax.broadcasted_iota(jnp.int32, (128, 512), 0) & 63) == which).astype(F32).astype(BF)
            lifted = lax.dot_general(hot, phl_v[...], (((0,), (0,)), ((), ())), preferred_element_type=F32)
            proj_v[512 * k : 512 * k + 512, :] = (interp_v[k].astype(F32) * lifted).astype(BF)
        if k0 == 0:
            for k in range(2, 8):
                coefs[k].start()
            table.start()
            pl.semaphore_wait(barrier, len(partners) + 2 * z)
            for dz in range(1, 4):

                @pl.when(z + dz >= 4)
                def _():
                    for dc in range(2):
                        pl.semaphore_signal(later, inc=1, device_id=device(x, y, z + dz, c + dc), device_id_type=MESH)

        for k in ks:
            if k < 7:
                for q in range(FIRST[k]):
                    piece(k, q).start()
    for (k, q), last in EXTRA:
        pl.when(z <= last)(piece(k, q).start)
    recv_v[:, pl.ds(pl.multiple_of(rad * 256, 256), 256)] = proj_v[3584:4096, :]

    for k in range(8):
        coefs[k].wait()
    part_v[...] = lax.dot_general(proj_v[...], coeffs_v[...], (((0,), (1,)), ((), ())), preferred_element_type=F32).astype(BF)

    @pl.when(z < 3)
    def _():
        pl.semaphore_wait(later, 6 - 2 * z)

    zc = [(dz, dc) for dz in (2, 1, 3, 0) for dc in (0, 1) if dz or dc]
    sums = []
    for i, (dz, dc) in enumerate(zc):
        to_slot = ((z + dz) % 4) * 2 + (c + dc) % 2
        src = part_v.at[pl.ds(pl.multiple_of(to_slot * 32, 32), 32), :]
        sums.append(send(src, rs_v.at[i], rss_sem.at[i], rsr_sem.at[i], (x, y, z + dz, c + dc)))
        sums[-1].start()
    a = lax.broadcasted_iota(jnp.int32, (480, 512), 0)
    b = lax.broadcasted_iota(jnp.int32, (480, 512), 1)
    low = b & 63
    perm_v[...] = jnp.where(low < 60, (a == (b >> 6) * 60 + low).astype(F32), 0.0).astype(BF)
    total = part_v[pl.ds(rows, 32), :].astype(F32)
    for i in range(7):
        sums[i].wait_recv()
        total = total + rs_v[i].astype(F32)
    xs_v[...] = total.astype(BF)
    pair = send(xs_v, xr_v, xx_sem.at[0], xx_sem.at[1], (x + 1 - 2 * xl, y, z, c))
    pair.start()
    for k, q in SECOND:
        piece(k, q).start()
    table.wait()
    pair.wait_recv()
    nodes = (xs_v[...].astype(F32) + xr_v[...].astype(F32)).astype(BF)
    turned = jnp.dot(nodes, table_v[...], preferred_element_type=F32).astype(BF)
    ang_v[y, xh, pl.ds(rows, 32), :] = jnp.dot(turned, perm_v[...], preferred_element_type=F32).astype(BF)

    def rows_of(i, dz):
        flip, dy = PLANE[i]
        at = pl.multiple_of((((z + dz) % 4) * 2 + c) * 32, 32)
        return ang_v.at[(y - dy) % 4, (xh + flip) % 2, pl.ds(at, 32), :]

    started = []

    def go(copy):
        copy.start()
        started.append(copy)

    def across(i):
        flip, dy = PLANE[i]
        to = (3 - x if flip else x, y + dy, z, c)
        return send(rows_of(0, 0), rows_of(0, 0), pls_sem.at[i], plr_sem.at[i], to)

    def along(i, step):
        n = 3 * i + (0 if step > 0 else 1)
        return send(rows_of(i, 0), rows_of(i, 0), zs_sem.at[n], zr_sem.at[n], (x, y, z + step, c))

    def relay(i):
        step = 1 if i % 2 else -1
        n = 3 * i + 2
        return send(rows_of(i, -step), rows_of(i, -step), zs_sem.at[n], zr_sem.at[n], (x, y, z + step, c))

    def other_core(i, dz):
        n = 4 * i + dz % 4
        return send(rows_of(i, dz), rows_of(i, dz), cs_sem.at[n], cr_sem.at[n], (x, y, z, c + 1))

    def near(i):
        step = 1 if i % 2 else -1
        along(i, step).wait_recv()
        go(relay(i))
        go(other_core(i, -step))
        along(i, -step).wait_recv()
        go(other_core(i, step))

    for i in (4, 1, 2, 5, 6, 3, 7):
        across(i).start()
    for step in (1, -1):
        go(along(0, step))
    go(other_core(0, 0))
    for i in (4, 1, 2, 5, 6, 3, 7):
        across(i).wait_send()
    for k, q in EARLY:
        piece(k, q).start()
    for i in range(8):
        if i:
            across(i).wait_recv()
            go(along(i, 1))
            go(along(i, -1))
            go(other_core(i, 0))
        if i == 7:
            for (k, q), last in EXTRA:
                pl.when(z > last)(piece(k, q).start)
        for k, q in THIRD.get(i, ()):
            piece(k, q).start()
        if i >= LAG:
            near(i - LAG)
    for i in range(8 - LAG, 8):
        near(i)
    for i in range(8):
        relay(i).wait_recv()
        go(other_core(i, 2))
    for i in range(8):
        for dz in range(4):
            other_core(i, dz).wait_recv()

    def back(k, h):
        dy, dx = OFF[k]
        half = slice(256 * h, 256 * h + 256)
        src = fsend_v.at[k // 2 * 2 + (xh + dx) % 2, :, half]
        to = (x + 2 * dx, y + dy, z, c)
        return send(src, frecv_v.at[k, :, half], fs_sem.at[2 * k + h], fr_sem.at[2 * k + h], to)

    for h in range(2):
        for k in range(7):
            for q in range(NQ[k] // 2 * h, NQ[k] // 2 * (h + 1)):
                piece(k, q).wait_recv()
        cols = [ang_v[:, :, :, pl.ds(pl.multiple_of(((y + dy) % 4) * 128, 128), 128)] for dy in (2, 1, 3, 0)]
        cols = jnp.concatenate([part.reshape(2048, 128) for part in cols], axis=1)
        res = jnp.dot(recv_v[256 * h : 256 * h + 256, :], cols, preferred_element_type=F32)
        fsend_v[:, :, 256 * h : 256 * h + 256] = res.astype(BF).T.reshape(8, 64, 256)
        for k in range(7):
            back(k, h).start()
    for h in range(2):
        for k in (7, 6, 5, 3, 4, 2, 1, 0):
            dy, dx = OFF[k]
            half = slice(256 * h, 256 * h + 256)
            if k < 7:
                back(k, h).wait_recv()
                block = frecv_v[k, :, half]
            else:
                block = fsend_v[6 + xh, :, half]
            source = ((y - dy) % 4) * 2 + (xh + dx) % 2
            out[:, pl.ds(pl.multiple_of(source * 512 + 256 * h, 256), 256)] = block[:60, :]

    for k in range(7):
        for q in range(NQ[k]):
            piece(k, q).wait_send()
        sums[k].wait_send()
        back(k, 0).wait_send()
        back(k, 1).wait_send()
    pair.wait_send()
    for copy in started:
        copy.wait_send()


def body(coeffs, interp, phases, tables, bins):
    dma = pltpu.SemaphoreType.DMA
    return pl.pallas_call(
        kernel,
        name="coupling",
        out_shape=pltpu.VMEM((60, 4096), BF),
        in_specs=[pl.BlockSpec(memory_space=pl.ANY)] * 5,
        out_specs=pl.BlockSpec(memory_space=pltpu.VMEM),
        scratch_shapes=[
            pltpu.VMEM((8, 512, 256), BF),
            pltpu.VMEM((480, 4096), BF),
            pltpu.VMEM((64, 256), F32),
            pltpu.VMEM((4096,), jnp.int32),
            pltpu.VMEM((480, 480), BF),
            pltpu.VMEM((128, 256), BF),
            pltpu.VMEM((480, 512), BF),
            pltpu.VMEM((4096, 256), BF),
            pltpu.VMEM((512, 2048), BF),
            pltpu.VMEM((480, 256), F32),
            pltpu.VMEM((256, 480), BF),
            pltpu.VMEM((7, 32, 480), BF),
            pltpu.VMEM((32, 480), BF),
            pltpu.VMEM((32, 480), BF),
            pltpu.VMEM((4, 2, 256, 512), BF),
            pltpu.VMEM((8, 64, 512), BF),
            pltpu.VMEM((7, 64, 512), BF),
            dma((8,)), dma((8,)), dma((3,)), dma((NPIECE,)), dma((NPIECE,)), dma((7,)), dma((7,)), dma((2,)),
            dma((8,)), dma((8,)), dma((24,)), dma((24,)), dma((32,)), dma((32,)), dma((14,)), dma((14,)), pltpu.SemaphoreType.REGULAR,
        ],
        compiler_params=pltpu.CompilerParams(
            collective_id=0, has_side_effects=True, vmem_limit_bytes=60 * 1024 * 1024
        ),
    )(coeffs.T, interp, phases, tables, bins).T


def solution(mesh):
    return jax.shard_map(
        body,
        mesh=mesh,
        in_specs=(P("sph", None), P("sph", "rad"), P(None, "rad"), P("rad", None, None), P("sph")),
        out_specs=P("sph", "rad"),
        check_vma=False,
    )
```

```python
import functools

import jax
import jax.numpy as jnp
from jax import lax
from jax.experimental import pallas as pl
from jax.experimental.pallas import tpu as pltpu
from jax.sharding import PartitionSpec as P

MESH = pl.DeviceIdType.MESH
BF = jnp.bfloat16
F32 = jnp.float32

OFF = [(2, 1), (2, 0), (1, 1), (1, 0), (3, 1), (3, 0), (0, 1), (0, 0)]
XK = [k for k, (dy, dx) in enumerate(OFF) if dx]
NQ = [4 if dx else 2 for dy, dx in OFF[:7]]
BASE = [sum(NQ[:k]) for k in range(7)]
NPIECE = sum(NQ)
FIRST = {0: 2, 1: 1, 2: 2, 3: 1, 4: 1, 5: 1, 6: 1}
SECOND = [(6, 1)]
REST = [(4, 1), (0, 2), (2, 2), (1, 1), (4, 2), (0, 3), (2, 3), (4, 3), (6, 3)]
THIRD = {7: REST}
PLANE = [(0, 0), (0, 1), (0, 3), (1, 0), (0, 2), (1, 1), (1, 3), (1, 2)]
LAG = 8
EARLY = [(3, 1), (5, 1)]
EXTRA = [((6, 2), 0)]
GROUP = 2


def where():
    s, r = lax.axis_index("sph"), lax.axis_index("rad")
    return (r % 2) * 2 + s // 8, r // 2, (s // 2) % 4, s % 2


def device(x, y, z, c):
    x, y, z, c = x % 4, y % 4, z % 4, c % 2
    return (x % 2) * 8 + z * 2 + c, y * 2 + x // 2


def kernel(
    coeffs, interp, phases, tables, bins, out,
    interp_v, coeffs_v, phases_v, bins_v, table_v, phl_v, perm_v, proj_v, recv_v, acc_v, part_v,
    rs_v, xs_v, xr_v, ang_v, fsend_v, frecv_v,
    in_sem, co_sem, small_sem, ps_sem, pr_sem, rss_sem, rsr_sem, xx_sem, pls_sem, plr_sem,
    zs_sem, zr_sem, cs_sem, cr_sem, fs_sem, fr_sem, later,
):
    x, y, z, c = where()
    xh, xl = x // 2, x % 2
    rad, slot = y * 2 + xh, z * 2 + c
    rows = pl.multiple_of(slot * 32, 32)

    def chunk_of(k):
        dy, dx = OFF[k]
        return ((y + dy) % 4) * 2 + (xh + dx) % 2

    loads = [
        pltpu.make_async_copy(phases, phases_v, small_sem.at[0]),
        pltpu.make_async_copy(bins, bins_v, small_sem.at[1]),
    ]
    inters, coefs = [], []
    for k in range(8):
        at = pl.ds(pl.multiple_of(chunk_of(k) * 512, 512), 512)
        inters.append(pltpu.make_async_copy(interp.at[at, :], interp_v.at[k], in_sem.at[k]))
        coefs.append(pltpu.make_async_copy(coeffs.at[:, at], coeffs_v.at[:, pl.ds(512 * k, 512)], co_sem.at[k]))
    table = pltpu.make_async_copy(tables.at[slot // 4], table_v, small_sem.at[2])

    partners = [(x + 2 * dx, y + dy, z, c) for dy, dx in OFF[:7]]
    partners += [(x, y, z, c + 1), (x + 1 - 2 * xl, y, z, c)]
    partners += [(3 - x, y + dy, z, c) for dy in range(4)]
    barrier = pltpu.get_barrier_semaphore()
    for partner in partners:
        pl.semaphore_signal(barrier, inc=1, device_id=device(*partner), device_id_type=MESH)
    for dz in range(1, 4):

        @pl.when(z + dz < 4)
        def _():
            for dc in range(2):
                pl.semaphore_signal(barrier, inc=1, device_id=device(x, y, z + dz, c + dc), device_id_type=MESH)

    for load in loads:
        load.start()

    for load in [*inters, *coefs[:2]]:
        load.start()
    for load in loads:
        load.wait()
    ph = phases_v[...]
    hi = ph.astype(BF)
    phl_v[0:64, :] = hi
    phl_v[64:128, :] = (ph - hi.astype(F32)).astype(BF)

    def send(src, dst, ssem, rsem, to):
        return pltpu.make_async_remote_copy(
            src_ref=src, dst_ref=dst, send_sem=ssem, recv_sem=rsem, device_id=device(*to), device_id_type=MESH
        )

    def piece(k, q):
        dy, dx = OFF[k]
        n = 512 // NQ[k]
        at = pl.ds(q * n, n)
        cols = pl.ds(pl.multiple_of(rad * 256, 256), 256)
        i = BASE[k] + q
        return send(proj_v.at[pl.ds(512 * k + q * n, n), :], recv_v.at[at, cols], ps_sem.at[i], pr_sem.at[i], (x + 2 * dx, y + dy, z, c))

    for k0 in range(0, 8, GROUP):
        ks = range(k0, k0 + GROUP)
        for k in ks:
            inters[k].wait()
        for k in ks:
            at = pl.ds(pl.multiple_of(chunk_of(k) * 512, 512), 512)
            which = bins_v[at][None, :]
            hot = ((lax.broadcasted_iota(jnp.int32, (128, 512), 0) & 63) == which).astype(F32).astype(BF)
            lifted = lax.dot_general(hot, phl_v[...], (((0,), (0,)), ((), ())), preferred_element_type=F32)
            proj_v[512 * k : 512 * k + 512, :] = (interp_v[k].astype(F32) * lifted).astype(BF)
        if k0 == 0:
            for k in range(2, 8):
                coefs[k].start()
            table.start()
            pl.semaphore_wait(barrier, len(partners) + 2 * z)
            for dz in range(1, 4):

                @pl.when(z + dz >= 4)
                def _():
                    for dc in range(2):
                        pl.semaphore_signal(later, inc=1, device_id=device(x, y, z + dz, c + dc), device_id_type=MESH)

        for k in ks:
            if k < 7:
                for q in range(FIRST[k]):
                    piece(k, q).start()
    for (k, q), last in EXTRA:
        pl.when(z <= last)(piece(k, q).start)
    recv_v[:, pl.ds(pl.multiple_of(rad * 256, 256), 256)] = proj_v[3584:4096, :]

    for k in range(8):
        coefs[k].wait()
    part_v[...] = lax.dot_general(proj_v[...], coeffs_v[...], (((0,), (1,)), ((), ())), preferred_element_type=F32).astype(BF)

    @pl.when(z < 3)
    def _():
        pl.semaphore_wait(later, 6 - 2 * z)

    zc = [(dz, dc) for dz in (2, 1, 3, 0) for dc in (0, 1) if dz or dc]
    sums = []
    for i, (dz, dc) in enumerate(zc):
        to_slot = ((z + dz) % 4) * 2 + (c + dc) % 2
        src = part_v.at[pl.ds(pl.multiple_of(to_slot * 32, 32), 32), :]
        sums.append(send(src, rs_v.at[i], rss_sem.at[i], rsr_sem.at[i], (x, y, z + dz, c + dc)))
        sums[-1].start()
    a = lax.broadcasted_iota(jnp.int32, (480, 512), 0)
    b = lax.broadcasted_iota(jnp.int32, (480, 512), 1)
    low = b & 63
    perm_v[...] = jnp.where(low < 60, (a == (b >> 6) * 60 + low).astype(F32), 0.0).astype(BF)
    total = part_v[pl.ds(rows, 32), :].astype(F32)
    for i in range(7):
        sums[i].wait_recv()
        total = total + rs_v[i].astype(F32)
    xs_v[...] = total.astype(BF)
    pair = send(xs_v, xr_v, xx_sem.at[0], xx_sem.at[1], (x + 1 - 2 * xl, y, z, c))
    pair.start()
    for k, q in SECOND:
        piece(k, q).start()
    table.wait()
    pair.wait_recv()
    nodes = (xs_v[...].astype(F32) + xr_v[...].astype(F32)).astype(BF)
    turned = jnp.dot(nodes, table_v[...], preferred_element_type=F32).astype(BF)
    ang_v[y, xh, pl.ds(rows, 32), :] = jnp.dot(turned, perm_v[...], preferred_element_type=F32).astype(BF)

    def rows_of(i, dz):
        flip, dy = PLANE[i]
        at = pl.multiple_of((((z + dz) % 4) * 2 + c) * 32, 32)
        return ang_v.at[(y - dy) % 4, (xh + flip) % 2, pl.ds(at, 32), :]

    started = []

    def go(copy):
        copy.start()
        started.append(copy)

    def across(i):
        flip, dy = PLANE[i]
        to = (3 - x if flip else x, y + dy, z, c)
        return send(rows_of(0, 0), rows_of(0, 0), pls_sem.at[i], plr_sem.at[i], to)

    def along(i, step):
        n = 3 * i + (0 if step > 0 else 1)
        return send(rows_of(i, 0), rows_of(i, 0), zs_sem.at[n], zr_sem.at[n], (x, y, z + step, c))

    def relay(i):
        step = 1 if i % 2 else -1
        n = 3 * i + 2
        return send(rows_of(i, -step), rows_of(i, -step), zs_sem.at[n], zr_sem.at[n], (x, y, z + step, c))

    def other_core(i, dz):
        n = 4 * i + dz % 4
        return send(rows_of(i, dz), rows_of(i, dz), cs_sem.at[n], cr_sem.at[n], (x, y, z, c + 1))

    def near(i):
        step = 1 if i % 2 else -1
        along(i, step).wait_recv()
        go(relay(i))
        go(other_core(i, -step))
        along(i, -step).wait_recv()
        go(other_core(i, step))

    for i in (4, 1, 2, 5, 6, 3, 7):
        across(i).start()
    for step in (1, -1):
        go(along(0, step))
    go(other_core(0, 0))
    for i in (4, 1, 2, 5, 6, 3, 7):
        across(i).wait_send()
    for k, q in EARLY:
        piece(k, q).start()
    for i in range(8):
        if i:
            across(i).wait_recv()
            go(along(i, 1))
            go(along(i, -1))
            go(other_core(i, 0))
        if i == 7:
            for (k, q), last in EXTRA:
                pl.when(z > last)(piece(k, q).start)
        for k, q in THIRD.get(i, ()):
            piece(k, q).start()
        if i >= LAG:
            near(i - LAG)
    for i in range(8 - LAG, 8):
        near(i)
    for i in range(8):
        relay(i).wait_recv()
        go(other_core(i, 2))
    for i in range(8):
        for dz in range(4):
            other_core(i, dz).wait_recv()

    def back(k, h):
        dy, dx = OFF[k]
        half = slice(256 * h, 256 * h + 256)
        src = fsend_v.at[k // 2 * 2 + (xh + dx) % 2, :, half]
        to = (x + 2 * dx, y + dy, z, c)
        return send(src, frecv_v.at[k, :, half], fs_sem.at[2 * k + h], fr_sem.at[2 * k + h], to)

    for h in range(2):
        for k in range(7):
            for q in range(NQ[k] // 2 * h, NQ[k] // 2 * (h + 1)):
                piece(k, q).wait_recv()
        cols = [ang_v[:, :, :, pl.ds(pl.multiple_of(((y + dy) % 4) * 128, 128), 128)] for dy in (2, 1, 3, 0)]
        cols = jnp.concatenate([part.reshape(2048, 128) for part in cols], axis=1)
        res = jnp.dot(recv_v[256 * h : 256 * h + 256, :], cols, preferred_element_type=F32)
        for b in range(2):
            part = res[:, 256 * b : 256 * b + 256].astype(BF).T
            fsend_v[4 * b : 4 * b + 4, :, 256 * h : 256 * h + 256] = part.reshape(4, 64, 256)
            for k in range(4 * b, min(4 * b + 4, 7)):
                back(k, h).start()
    for h in range(2):
        for k in (7, 5, 3, 6, 1, 4, 2, 0):
            dy, dx = OFF[k]
            half = slice(256 * h, 256 * h + 256)
            if k < 7:
                back(k, h).wait_recv()
                block = frecv_v[k, :, half]
            else:
                block = fsend_v[6 + xh, :, half]
            source = ((y - dy) % 4) * 2 + (xh + dx) % 2
            out[:, pl.ds(pl.multiple_of(source * 512 + 256 * h, 256), 256)] = block[:60, :]

    for k in range(7):
        for q in range(NQ[k]):
            piece(k, q).wait_send()
        sums[k].wait_send()
        back(k, 0).wait_send()
        back(k, 1).wait_send()
    pair.wait_send()
    for copy in started:
        copy.wait_send()


def body(coeffs, interp, phases, tables, bins):
    dma = pltpu.SemaphoreType.DMA
    return pl.pallas_call(
        kernel,
        name="coupling",
        out_shape=pltpu.VMEM((60, 4096), BF),
        in_specs=[pl.BlockSpec(memory_space=pl.ANY)] * 5,
        out_specs=pl.BlockSpec(memory_space=pltpu.VMEM),
        scratch_shapes=[
            pltpu.VMEM((8, 512, 256), BF),
            pltpu.VMEM((480, 4096), BF),
            pltpu.VMEM((64, 256), F32),
            pltpu.VMEM((4096,), jnp.int32),
            pltpu.VMEM((480, 480), BF),
            pltpu.VMEM((128, 256), BF),
            pltpu.VMEM((480, 512), BF),
            pltpu.VMEM((4096, 256), BF),
            pltpu.VMEM((512, 2048), BF),
            pltpu.VMEM((480, 256), F32),
            pltpu.VMEM((256, 480), BF),
            pltpu.VMEM((7, 32, 480), BF),
            pltpu.VMEM((32, 480), BF),
            pltpu.VMEM((32, 480), BF),
            pltpu.VMEM((4, 2, 256, 512), BF),
            pltpu.VMEM((8, 64, 512), BF),
            pltpu.VMEM((7, 64, 512), BF),
            dma((8,)), dma((8,)), dma((3,)), dma((NPIECE,)), dma((NPIECE,)), dma((7,)), dma((7,)), dma((2,)),
            dma((8,)), dma((8,)), dma((24,)), dma((24,)), dma((32,)), dma((32,)), dma((14,)), dma((14,)), pltpu.SemaphoreType.REGULAR,
        ],
        compiler_params=pltpu.CompilerParams(
            collective_id=0, has_side_effects=True, vmem_limit_bytes=60 * 1024 * 1024
        ),
    )(coeffs.T, interp, phases, tables, bins).T


def solution(mesh):
    return jax.shard_map(
        body,
        mesh=mesh,
        in_specs=(P("sph", None), P("sph", "rad"), P(None, "rad"), P("rad", None, None), P("sph")),
        out_specs=P("sph", "rad"),
        check_vma=False,
    )
```

```python
import functools

import jax
import jax.numpy as jnp
from jax import lax
from jax.experimental import pallas as pl
from jax.experimental.pallas import tpu as pltpu
from jax.sharding import PartitionSpec as P

MESH = pl.DeviceIdType.MESH
BF = jnp.bfloat16
F32 = jnp.float32

OFF = [(2, 1), (2, 0), (1, 1), (1, 0), (3, 1), (3, 0), (0, 1), (0, 0)]
XK = [k for k, (dy, dx) in enumerate(OFF) if dx]
NQ = [4 if dx else 2 for dy, dx in OFF[:7]]
BASE = [sum(NQ[:k]) for k in range(7)]
NPIECE = sum(NQ)
FIRST = {0: 2, 1: 1, 2: 2, 3: 1, 4: 1, 5: 1, 6: 1}
SECOND = [(6, 1)]
REST = [(4, 1), (0, 2), (2, 2), (1, 1), (4, 2), (0, 3), (2, 3), (4, 3), (6, 3)]
THIRD = {7: REST}
PLANE = [(0, 0), (0, 1), (0, 3), (1, 0), (0, 2), (1, 1), (1, 3), (1, 2)]
LAG = 8
EARLY = [(3, 1), (5, 1)]
EXTRA = [((6, 2), 0)]
GROUP = 2


def where():
    s, r = lax.axis_index("sph"), lax.axis_index("rad")
    return (r % 2) * 2 + s // 8, r // 2, (s // 2) % 4, s % 2


def device(x, y, z, c):
    x, y, z, c = x % 4, y % 4, z % 4, c % 2
    return (x % 2) * 8 + z * 2 + c, y * 2 + x // 2


def kernel(
    coeffs, interp, phases, tables, bins, out,
    interp_v, coeffs_v, phases_v, bins_v, table_v, phl_v, perm_v, proj_v, recv_v, acc_v, part_v,
    rs_v, xs_v, xr_v, ang_v, fsend_v, frecv_v,
    in_sem, co_sem, small_sem, ps_sem, pr_sem, rss_sem, rsr_sem, xx_sem, pls_sem, plr_sem,
    zs_sem, zr_sem, cs_sem, cr_sem, fs_sem, fr_sem, later,
):
    x, y, z, c = where()
    xh, xl = x // 2, x % 2
    rad, slot = y * 2 + xh, z * 2 + c
    rows = pl.multiple_of(slot * 32, 32)

    def chunk_of(k):
        dy, dx = OFF[k]
        return ((y + dy) % 4) * 2 + (xh + dx) % 2

    loads = [
        pltpu.make_async_copy(phases, phases_v, small_sem.at[0]),
        pltpu.make_async_copy(bins, bins_v, small_sem.at[1]),
    ]
    inters, coefs = [], []
    for k in range(8):
        at = pl.ds(pl.multiple_of(chunk_of(k) * 512, 512), 512)
        inters.append(pltpu.make_async_copy(interp.at[at, :], interp_v.at[k], in_sem.at[k]))
        coefs.append(pltpu.make_async_copy(coeffs.at[:, at], coeffs_v.at[:, pl.ds(512 * k, 512)], co_sem.at[k]))
    table = pltpu.make_async_copy(tables.at[slot // 4], table_v, small_sem.at[2])

    partners = [(x + 2 * dx, y + dy, z, c) for dy, dx in OFF[:7]]
    partners += [(x, y, z, c + 1), (x + 1 - 2 * xl, y, z, c)]
    partners += [(3 - x, y + dy, z, c) for dy in range(4)]
    barrier = pltpu.get_barrier_semaphore()
    for partner in partners:
        pl.semaphore_signal(barrier, inc=1, device_id=device(*partner), device_id_type=MESH)
    for dz in range(1, 4):

        @pl.when(z + dz < 4)
        def _():
            for dc in range(2):
                pl.semaphore_signal(barrier, inc=1, device_id=device(x, y, z + dz, c + dc), device_id_type=MESH)

    for load in loads:
        load.start()

    for load in [*inters, *coefs[:2]]:
        load.start()
    for load in loads:
        load.wait()
    ph = phases_v[...]
    hi = ph.astype(BF)
    phl_v[0:64, :] = hi
    phl_v[64:128, :] = (ph - hi.astype(F32)).astype(BF)

    def send(src, dst, ssem, rsem, to):
        return pltpu.make_async_remote_copy(
            src_ref=src, dst_ref=dst, send_sem=ssem, recv_sem=rsem, device_id=device(*to), device_id_type=MESH
        )

    def piece(k, q):
        dy, dx = OFF[k]
        n = 512 // NQ[k]
        at = pl.ds(q * n, n)
        cols = pl.ds(pl.multiple_of(rad * 256, 256), 256)
        i = BASE[k] + q
        return send(proj_v.at[pl.ds(512 * k + q * n, n), :], recv_v.at[at, cols], ps_sem.at[i], pr_sem.at[i], (x + 2 * dx, y + dy, z, c))

    for k0 in range(0, 8, GROUP):
        ks = range(k0, k0 + GROUP)
        for k in ks:
            inters[k].wait()
        for k in ks:
            at = pl.ds(pl.multiple_of(chunk_of(k) * 512, 512), 512)
            which = bins_v[at][None, :]
            hot = ((lax.broadcasted_iota(jnp.int32, (128, 512), 0) & 63) == which).astype(F32).astype(BF)
            lifted = lax.dot_general(hot, phl_v[...], (((0,), (0,)), ((), ())), preferred_element_type=F32)
            proj_v[512 * k : 512 * k + 512, :] = (interp_v[k].astype(F32) * lifted).astype(BF)
        if k0 == 0:
            for k in range(2, 8):
                coefs[k].start()
            table.start()
            pl.semaphore_wait(barrier, len(partners) + 2 * z)
            for dz in range(1, 4):

                @pl.when(z + dz >= 4)
                def _():
                    for dc in range(2):
                        pl.semaphore_signal(later, inc=1, device_id=device(x, y, z + dz, c + dc), device_id_type=MESH)

        for k in ks:
            if k < 7:
                for q in range(FIRST[k]):
                    piece(k, q).start()
    for (k, q), last in EXTRA:
        pl.when(z <= last)(piece(k, q).start)
    recv_v[:, pl.ds(pl.multiple_of(rad * 256, 256), 256)] = proj_v[3584:4096, :]

    for k in range(8):
        coefs[k].wait()
    part_v[...] = lax.dot_general(proj_v[...], coeffs_v[...], (((0,), (1,)), ((), ())), preferred_element_type=F32).astype(BF)

    @pl.when(z < 3)
    def _():
        pl.semaphore_wait(later, 6 - 2 * z)

    zc = [(dz, dc) for dz in (2, 1, 3, 0) for dc in (0, 1) if dz or dc]
    sums = []
    for i, (dz, dc) in enumerate(zc):
        to_slot = ((z + dz) % 4) * 2 + (c + dc) % 2
        src = part_v.at[pl.ds(pl.multiple_of(to_slot * 32, 32), 32), :]
        sums.append(send(src, rs_v.at[i], rss_sem.at[i], rsr_sem.at[i], (x, y, z + dz, c + dc)))
        sums[-1].start()
    total = part_v[pl.ds(rows, 32), :].astype(F32)
    sums[0].wait_recv()
    a = lax.broadcasted_iota(jnp.int32, (480, 512), 0)
    b = lax.broadcasted_iota(jnp.int32, (480, 512), 1)
    low = b & 63
    perm_v[...] = jnp.where(low < 60, (a == (b >> 6) * 60 + low).astype(F32), 0.0).astype(BF)
    for i in range(7):
        if i:
            sums[i].wait_recv()
        total = total + rs_v[i].astype(F32)
    xs_v[...] = total.astype(BF)
    pair = send(xs_v, xr_v, xx_sem.at[0], xx_sem.at[1], (x + 1 - 2 * xl, y, z, c))
    pair.start()
    for k, q in SECOND:
        piece(k, q).start()
    table.wait()
    pair.wait_recv()
    nodes = (xs_v[...].astype(F32) + xr_v[...].astype(F32)).astype(BF)
    turned = jnp.dot(nodes, table_v[...], preferred_element_type=F32).astype(BF)
    ang_v[y, xh, pl.ds(rows, 32), :] = jnp.dot(turned, perm_v[...], preferred_element_type=F32).astype(BF)

    def rows_of(i, dz):
        flip, dy = PLANE[i]
        at = pl.multiple_of((((z + dz) % 4) * 2 + c) * 32, 32)
        return ang_v.at[(y - dy) % 4, (xh + flip) % 2, pl.ds(at, 32), :]

    started = []

    def go(copy):
        copy.start()
        started.append(copy)

    def across(i):
        flip, dy = PLANE[i]
        to = (3 - x if flip else x, y + dy, z, c)
        return send(rows_of(0, 0), rows_of(0, 0), pls_sem.at[i], plr_sem.at[i], to)

    def along(i, step):
        n = 3 * i + (0 if step > 0 else 1)
        return send(rows_of(i, 0), rows_of(i, 0), zs_sem.at[n], zr_sem.at[n], (x, y, z + step, c))

    def relay(i):
        step = 1 if i % 2 else -1
        n = 3 * i + 2
        return send(rows_of(i, -step), rows_of(i, -step), zs_sem.at[n], zr_sem.at[n], (x, y, z + step, c))

    def other_core(i, dz):
        n = 4 * i + dz % 4
        return send(rows_of(i, dz), rows_of(i, dz), cs_sem.at[n], cr_sem.at[n], (x, y, z, c + 1))

    def near(i):
        step = 1 if i % 2 else -1
        along(i, step).wait_recv()
        go(relay(i))
        go(other_core(i, -step))
        along(i, -step).wait_recv()
        go(other_core(i, step))

    for i in (4, 1, 2, 5, 6, 3, 7):
        across(i).start()
    for step in (1, -1):
        go(along(0, step))
    go(other_core(0, 0))
    for i in (4, 1, 2, 5, 6, 3, 7):
        across(i).wait_send()
    for k, q in EARLY:
        piece(k, q).start()
    for i in range(8):
        if i:
            across(i).wait_recv()
            go(along(i, 1))
            go(along(i, -1))
            go(other_core(i, 0))
        if i == 7:
            for (k, q), last in EXTRA:
                pl.when(z > last)(piece(k, q).start)
        for k, q in THIRD.get(i, ()):
            piece(k, q).start()
        if i >= LAG:
            near(i - LAG)
    for i in range(8 - LAG, 8):
        near(i)
    for i in range(8):
        relay(i).wait_recv()
        go(other_core(i, 2))
    for i in range(8):
        for dz in range(4):
            other_core(i, dz).wait_recv()

    def back(k, h):
        dy, dx = OFF[k]
        half = slice(256 * h, 256 * h + 256)
        src = fsend_v.at[k // 2 * 2 + (xh + dx) % 2, :, half]
        to = (x + 2 * dx, y + dy, z, c)
        return send(src, frecv_v.at[k, :, half], fs_sem.at[2 * k + h], fr_sem.at[2 * k + h], to)

    for h in range(2):
        for k in range(7):
            for q in range(NQ[k] // 2 * h, NQ[k] // 2 * (h + 1)):
                piece(k, q).wait_recv()
        cols = [ang_v[:, :, :, pl.ds(pl.multiple_of(((y + dy) % 4) * 128, 128), 128)] for dy in (2, 1, 3, 0)]
        cols = jnp.concatenate([part.reshape(2048, 128) for part in cols], axis=1)
        res = jnp.dot(recv_v[256 * h : 256 * h + 256, :], cols, preferred_element_type=F32)
        fsend_v[:, :, 256 * h : 256 * h + 256] = res.astype(BF).T.reshape(8, 64, 256)
        for k in range(7):
            back(k, h).start()
    for h in range(2):
        for k in (7, 5, 3, 6, 1, 4, 2, 0):
            dy, dx = OFF[k]
            half = slice(256 * h, 256 * h + 256)
            if k < 7:
                back(k, h).wait_recv()
                block = frecv_v[k, :, half]
            else:
                block = fsend_v[6 + xh, :, half]
            source = ((y - dy) % 4) * 2 + (xh + dx) % 2
            out[:, pl.ds(pl.multiple_of(source * 512 + 256 * h, 256), 256)] = block[:60, :]

    for k in range(7):
        for q in range(NQ[k]):
            piece(k, q).wait_send()
        sums[k].wait_send()
        back(k, 0).wait_send()
        back(k, 1).wait_send()
    pair.wait_send()
    for copy in started:
        copy.wait_send()


def body(coeffs, interp, phases, tables, bins):
    dma = pltpu.SemaphoreType.DMA
    return pl.pallas_call(
        kernel,
        name="coupling",
        out_shape=pltpu.VMEM((60, 4096), BF),
        in_specs=[pl.BlockSpec(memory_space=pl.ANY)] * 5,
        out_specs=pl.BlockSpec(memory_space=pltpu.VMEM),
        scratch_shapes=[
            pltpu.VMEM((8, 512, 256), BF),
            pltpu.VMEM((480, 4096), BF),
            pltpu.VMEM((64, 256), F32),
            pltpu.VMEM((4096,), jnp.int32),
            pltpu.VMEM((480, 480), BF),
            pltpu.VMEM((128, 256), BF),
            pltpu.VMEM((480, 512), BF),
            pltpu.VMEM((4096, 256), BF),
            pltpu.VMEM((512, 2048), BF),
            pltpu.VMEM((480, 256), F32),
            pltpu.VMEM((256, 480), BF),
            pltpu.VMEM((7, 32, 480), BF),
            pltpu.VMEM((32, 480), BF),
            pltpu.VMEM((32, 480), BF),
            pltpu.VMEM((4, 2, 256, 512), BF),
            pltpu.VMEM((8, 64, 512), BF),
            pltpu.VMEM((7, 64, 512), BF),
            dma((8,)), dma((8,)), dma((3,)), dma((NPIECE,)), dma((NPIECE,)), dma((7,)), dma((7,)), dma((2,)),
            dma((8,)), dma((8,)), dma((24,)), dma((24,)), dma((32,)), dma((32,)), dma((14,)), dma((14,)), pltpu.SemaphoreType.REGULAR,
        ],
        compiler_params=pltpu.CompilerParams(
            collective_id=0, has_side_effects=True, vmem_limit_bytes=60 * 1024 * 1024
        ),
    )(coeffs.T, interp, phases, tables, bins).T


def solution(mesh):
    return jax.shard_map(
        body,
        mesh=mesh,
        in_specs=(P("sph", None), P("sph", "rad"), P(None, "rad"), P("rad", None, None), P("sph")),
        out_specs=P("sph", "rad"),
        check_vma=False,
    )
```
